512 devices in a mesh: ga: 128 (over z, y, core), band: 4 (over x).
Axes of the slice: x: 4, y: 8, z: 8, core: 2. Of those that a mesh axis runs over, the one named last changes fastest.
Arguments:
- coeffs: bfloat16 [32768, 128], P('ga', 'band'), may hold values from -6 to 6
- coupling: bfloat16 [12288, 12288], P('ga', 'band'), may hold values from -0.21875 to 0.21875
- miller: int32 [3, 32768], P(None, 'ga'), may hold values from -24 to 24
- species: int32 [1024], replicated, may hold values from 0 to 3
- proj_atom: int32 [12288], replicated, may hold values from 0 to 1023, as said below
- positions: float32 [3, 1024], replicated, may hold values from 0 to 1
- radial: float32 [12, 128], replicated, may hold values from -8 to 8
Outputs:
- result: bfloat16 [32768, 128], P('ga', 'band')
The draws below stay inside these ranges and needn't reach their ends.
Inputs may be any that keep to these rules, and one draw needn't show every extreme that they name: `proj_atom`: projector p has channel p mod 12; each atom owns 12 consecutive projectors.
All inputs are finite; a program needn't handle non-finite values.
Results may differ from the reference program's by a relative error of at most 0.008.
Values may be sent and summed in bfloat16 or wider, within the bound.
A program may use at most 64 MiB of HBM per device.

```python
import math
import jax
import jax.numpy as jnp
from jax import lax

ATOMS = 1024
NCH = 12
SHELLS = 3
KINDS = 4
QBINS = 128
MMAX = 24
PWD = 256
NPROJ = 12288
NPW = 32768
NBANDS = 128


def draw_proj_atom(key, part):
    order = jax.random.permutation(jax.random.fold_in(key, 17), ATOMS).astype(jnp.int32)
    return jnp.repeat(order, NCH).astype(jnp.int32)


def touch_ends(drawn, rng, low, high):
    shape = drawn.shape
    index_at = [jax.random.randint(jax.random.fold_in(rng, axis), (), 0, shape[axis]) for axis in range(len(shape))]
    drawn = drawn.at[tuple(index_at)].set(low)
    longest = shape.index(max(shape))
    index_at[longest] = (index_at[longest] + 1) % shape[longest]
    return drawn.at[tuple(index_at)].set(high)


def steps_of(stream_key, dims, pieces, low, high):
    gain = 1.0
    for axis_at, shards_of in pieces:
        steps = jax.random.uniform(jax.random.fold_in(jax.random.fold_in(stream_key, 6), axis_at), (shards_of,), jnp.float32, low / len(pieces), high / len(pieces))
        gain = gain * jnp.repeat(jnp.exp(steps), dims[axis_at] // shards_of).reshape((-1,) + (1,) * (len(dims) - 1 - axis_at))
    return gain


def centred(stream_key, extent, width, limit, split=(), held_as=jnp.bfloat16):
    factor_of = steps_of(stream_key, extent, split, -0.22, 0.18) if split else 1.0
    array = jax.random.normal(stream_key, extent, jnp.float32) * width * factor_of
    return jnp.minimum(jnp.maximum(array, -limit), limit).astype(held_as)


def setup_inputs(seed: int = 0) -> dict:
    splits = jax.random.split(jax.random.key(seed), 8)
    return {
        "coeffs": centred(splits[0], (NPW, NBANDS), 1.0, 6.0, ((0, 128), (1, 4))),
        "coupling": centred(splits[1], (NPROJ, NPROJ), (NPROJ // 16) ** -0.5, 0.21875, ((0, 128), (1, 4))),
        "miller": touch_ends(jax.random.randint(splits[2], (3, NPW), 0 - MMAX, MMAX + 1), jax.random.fold_in(splits[2], 1), 0 - MMAX, MMAX).astype(jnp.int32),
        "species": touch_ends(jax.random.randint(splits[3], (ATOMS,), 0, KINDS), jax.random.fold_in(splits[3], 1), 0, KINDS - 1).astype(jnp.int32),
        "proj_atom": draw_proj_atom(jax.random.fold_in(splits[7], 71), 0),
        "positions": jnp.clip(jax.random.uniform(splits[5], (3, ATOMS), jnp.float32, 0.0, 1.0), 0.0, 1.0),
        "radial": centred(splits[6], (KINDS * SHELLS, QBINS), 1.5, 8.0, (), jnp.float32),
    }


def radial_values(miller_block, radial):
    mf = miller_block.astype(jnp.float32)
    qval = (mf[0] * mf[0] + mf[1] * mf[1] + mf[2] * mf[2]) * ((QBINS - 1) / (3.0 * MMAX * MMAX))
    knots = jnp.arange(QBINS, dtype=jnp.int32).astype(jnp.float32)
    hats = jnp.maximum(0.0, 1.0 - jnp.abs(qval[:, None] - knots[None, :]))
    return jnp.dot(hats, radial.T, precision=lax.Precision.HIGHEST)

def make_beta(miller_block, radval, species, proj_atom, positions, start, count, scale):
    mf = miller_block.astype(jnp.float32)
    atoms = lax.dynamic_slice_in_dim(proj_atom, jnp.asarray(start).astype(jnp.int32), count)
    channel = (jnp.asarray(start).astype(jnp.int32) + jnp.arange(count, dtype=jnp.int32)) % NCH
    shell = channel // 4
    comp = channel % 4
    kind = jnp.take(species, atoms)
    column = kind * SHELLS + shell
    select = (column[None, :] == jnp.arange(KINDS * SHELLS, dtype=jnp.int32)[:, None]).astype(jnp.float32)
    radpart = jnp.dot(radval, select, precision=lax.Precision.HIGHEST)
    place = jnp.take(positions, atoms, axis=1)
    theta = 2.0 * math.pi * (mf[0][:, None] * place[0][None, :] + mf[1][:, None] * place[1][None, :] + mf[2][:, None] * place[2][None, :])
    unit = mf / MMAX
    angular = jnp.where(comp[None, :] == 1, unit[0][:, None], jnp.where(comp[None, :] == 2, unit[1][:, None], jnp.where(comp[None, :] == 3, unit[2][:, None], jnp.ones_like(theta))))
    phase = jnp.where(comp[None, :] == 0, jnp.cos(theta), jnp.sin(theta))
    return (radpart * angular * phase * scale).astype(jnp.bfloat16)

def reference(coeffs, coupling, miller, species, proj_atom, positions, radial):
    scale = 1.0 / math.sqrt(NPW)
    blocks = NPW // PWD
    miller_blocks = miller.reshape(3, blocks, PWD).transpose(1, 0, 2)
    coeff_blocks = coeffs.reshape(blocks, PWD, NBANDS)

    def project(total, item):
        mblock, cblock = item
        radval = radial_values(mblock, radial)
        beta = make_beta(mblock, radval, species, proj_atom, positions, 0, NPROJ, scale)
        term = lax.dot_general(beta, cblock, (((0,), (0,)), ((), ())), preferred_element_type=jnp.float32)
        return (total + term, None)
    proj, unused = lax.scan(project, jnp.zeros((NPROJ, NBANDS), jnp.float32), (miller_blocks, coeff_blocks))
    proj_b = proj.astype(jnp.bfloat16)
    mixed = jnp.dot(coupling, proj_b, preferred_element_type=jnp.float32).astype(jnp.bfloat16)

    def addback(carry, item):
        mblock, cblock = item
        radval = radial_values(mblock, radial)
        beta = make_beta(mblock, radval, species, proj_atom, positions, 0, NPROJ, scale)
        out = cblock.astype(jnp.float32) + jnp.dot(beta, mixed, preferred_element_type=jnp.float32)
        return (carry, out.astype(jnp.bfloat16))
    unused, outs = lax.scan(addback, jnp.zeros((), jnp.float32), (miller_blocks, coeff_blocks))
    return outs.reshape(NPW, NBANDS)
```

```python
import math

import jax
import jax.numpy as jnp
from jax import lax
from jax.experimental import pallas as pl
from jax.experimental.pallas import tpu as pltpu
from jax.sharding import Mesh
from jax.sharding import PartitionSpec as P

NCH = 12
QBINS = 128
MMAX = 24
GA = ("z", "y", "core")
NZ, NY, NC, NX = 8, 8, 2, 4
PW = 256
BANDS = 32
ATOMS = 1024
LANE_ATOMS = 128
WIDTH = LANE_ATOMS * NCH
HALF = 6144
SCALE = 1.0 / math.sqrt(32768.0)
MESH = pl.DeviceIdType.MESH
FAR_FIRST = (4, 3, 5, 2, 6, 1, 7)
NEAR_FIRST = (1, 7, 2, 6, 3, 5, 4)
F32 = jnp.float32
BF16 = jnp.bfloat16


def dot(a, b, **kw):
    return jnp.dot(a, b, preferred_element_type=F32, **kw)


def split2(v):
    hi = v.astype(BF16)
    return hi, (v - hi.astype(F32)).astype(BF16)


def iota(shape, dim):
    return lax.broadcasted_iota(jnp.int32, shape, dim)


def horner(y, terms):
    acc = jnp.full_like(y, terms[-1])
    for term in terms[-2::-1]:
        acc = acc * y + term
    return acc


SIN_TERMS = [(-1) ** k * math.pi ** (2 * k + 1) / math.factorial(2 * k + 1) for k in range(6)]
COS_TERMS = [(-1) ** k * math.pi ** (2 * k) / math.factorial(2 * k) for k in range(6)]


def circle(turns):
    r = turns - jnp.floor(turns + 0.5)
    y = r * r
    s = r * horner(y, SIN_TERMS)
    c = horner(y, COS_TERMS)
    return 1.0 - 2.0 * s * s, 2.0 * s * c


def fold(v):
    v = v + pltpu.roll(v, 32, 1)
    return v + pltpu.roll(v, 64, 1)


def kernel(
    coeffs, miller, owner, species, positions, radial, coupling, out,
    cbuf, mtmp, beta, acc, place, rad_hi, rad_lo, sel_a, expand, own_f,
    rs_send, rs_recv, nbuf, wide, ball, xsend, xrecv, mx, fsend, frecv,
    a_s, a_r, rs_s, rs_r, g1_s, g1_r, g2_s, g2_r, b_s, b_r, b_l, x_s, x_r, e_s, e_r, f_s, f_r,
):
    z, y, c, x = (lax.axis_index(a) for a in ("z", "y", "core", "band"))
    barrier = pltpu.get_barrier_semaphore()

    def signal(to):
        pl.semaphore_signal(barrier, inc=1, device_id=to, device_id_type=MESH)

    for d in FAR_FIRST:
        signal((z, (y + d) % NY, c, x))
        for o in range(NC):
            signal(((z + d) % NZ, y, (c + o) % NC, x))
    for d in (2, 1, 3):
        for o in range(NC):
            signal((z, y, (c + o) % NC, (x + d) % NX))
    signal((z, y, 1 - c, x))
    greeted = 7 + 14 + 6 + 1

    def remote(src, dst, s, r, to):
        return pltpu.make_async_remote_copy(
            src_ref=src, dst_ref=dst, send_sem=s, recv_sem=r, device_id=to, device_id_type=MESH
        )

    mtmp[...] = jnp.zeros_like(mtmp)
    mtmp[0:3, :] = miller[...].astype(F32)
    cbuf[y, 0:32, :] = coeffs[...].astype(F32).T.astype(BF16)
    cbuf[y, 32:40, :] = mtmp[...].astype(BF16)

    col = iota((128, 128), 1)
    j, q, i = col >> 5, (col >> 1) & 15, col & 1
    first = NCH * ((((q >> 1) * NY + y) * NC + (q & 1)) * 8 + j * 2 + i)
    row_of, lane_of = first >> 7, first & 127
    ids = owner[...].astype(F32).T
    ids_hi = jnp.floor(ids * (1.0 / 32.0))
    ids_lo = ids - 32.0 * ids_hi
    pick = (iota((128, 128), 0) == row_of).astype(F32)[0:96, :].astype(BF16)
    at_row = 32.0 * dot(ids_hi.astype(BF16), pick) + dot(ids_lo.astype(BF16), pick)
    atom = jnp.sum(jnp.where(iota((128, 128), 0) == lane_of, at_row, 0.0), axis=0, keepdims=True)
    onehot = (iota((ATOMS, 128), 0) == atom.astype(jnp.int32)).astype(F32)
    place[...] = dot(positions[...], onehot, precision=lax.Precision.HIGHEST)
    kind = dot(species[...].astype(F32).astype(BF16), onehot.astype(BF16))

    atom_row = iota((128, WIDTH), 0)
    lane = iota((128, WIDTH), 1)
    off = lane - NCH * atom_row
    spread = ((off >= 0) & (off < NCH)).astype(F32).astype(BF16)
    kind_at = dot(kind.astype(BF16), spread)
    lane1 = iota((1, WIDTH), 1)
    chan = lane1 - NCH * jnp.floor((lane1.astype(F32) + 0.5) * (1.0 / NCH)).astype(jnp.int32)
    column = kind_at.astype(jnp.int32) * 3 + (chan >> 2)
    sel_a[...] = (
        ((atom_row & 15) == column) & (((atom_row >> 4) & 3) == (chan & 3))
    ).astype(F32).astype(BF16)

    krow = iota((256, WIDTH // 2), 0)
    klane = iota((256, WIDTH // 2), 1)
    koff = klane - NCH * (krow & 63)
    expand[...] = (
        (koff >= 0) & (koff < NCH) & (((koff & 3) == 0) == (krow < 128))
    ).astype(F32).astype(BF16)

    rsel = ((iota((128, 12), 0) & 15) == iota((128, 12), 1)).astype(F32)
    rad = dot(rsel, radial[...], precision=lax.Precision.HIGHEST).T
    hi, lo = split2(rad)
    rad_hi[...] = hi
    rad_lo[...] = lo
    acc[...] = jnp.zeros_like(acc)

    def part_y(yy):
        return cbuf.at[yy]

    def make_block(yy):
        m8 = mtmp[...]
        n2 = jnp.sum(m8 * m8, axis=0, keepdims=True)
        qv = n2 * ((QBINS - 1) / (3.0 * MMAX * MMAX))
        mt = jnp.where(iota((8, PW), 0) == 3, qv, m8).T
        lanes = iota((PW, 128), 1)
        m0, m1, m2, qcol = (
            jnp.broadcast_to(mt[:, k : k + 1], (PW, 128)) for k in range(4)
        )
        hats = jnp.maximum(0.0, 1.0 - jnp.abs(qcol - lanes.astype(F32)))
        h_hi, h_lo = split2(hats)
        radval = dot(h_hi, rad_hi[...]) + dot(h_lo, rad_hi[...]) + dot(h_hi, rad_lo[...])
        t = (lanes >> 4) & 3
        w = jnp.where(t == 1, m0, jnp.where(t == 2, m1, m2)) * (SCALE / MMAX)
        amp = radval * jnp.where(t == 0, SCALE, w)
        a_hi, a_lo = split2(amp)
        amp2 = jnp.where(lanes < 64, a_hi.astype(F32), a_lo.astype(F32)).astype(BF16)
        turns = m0 * place[0:1, :] + m1 * place[1:2, :] + m2 * place[2:3, :]
        cos, sin = circle(turns)
        parts = []
        for v in (cos, sin):
            vh = v.astype(BF16).astype(F32)
            vl = pltpu.roll(v - vh, 64, 1)
            parts.append((jnp.where(lanes < 64, vh, vl), jnp.where(lanes < 64, vl, vh)))
        for h in range(2):
            lhs = jnp.concatenate([parts[0][h], parts[1][h]], axis=1).astype(BF16)
            cols = slice(h * (WIDTH // 2), (h + 1) * (WIDTH // 2))
            phase = dot(lhs, expand[...])
            ampl = dot(amp2, sel_a[:, cols])
            block = (phase * ampl).astype(BF16)
            beta[yy, :, cols] = block
            acc[:, cols] += dot(cbuf[yy, 0:32, :], block)

    make_block(y)

    pl.semaphore_wait(barrier, greeted)
    a_out = []
    for d in FAR_FIRST:
        yy = (y + d) % NY
        cp = remote(part_y(y), part_y(y), a_s.at[d], a_r.at[y], (z, yy, c, x))
        cp.start()
        a_out.append(cp)

    side = x // 2
    slot = (x % 2) * NC + c
    home = ball.at[x % 2, pl.ds(96 * c, 96)]
    b_out = []
    for d in (2, 1, 3):
        cp = remote(coupling, home, b_s.at[d], b_r.at[slot], (z, y, side, (x + d) % NX))
        cp.start()
        b_out.append(cp)
    own_copy = pltpu.make_async_copy(coupling, home, b_l)
    partner_copy = remote(coupling, home, b_s.at[0], b_r.at[slot], (z, y, 1 - c, x))

    @pl.when(side == c)
    def _():
        own_copy.start()

    @pl.when(side != c)
    def _():
        partner_copy.start()

    def step(k, carry):
        d = jnp.where(k % 2 == 1, (k + 1) // 2, NY - k // 2)
        yy = (y + d) % NY
        remote(part_y(yy), part_y(yy), a_s.at[0], a_r.at[yy], (z, y, c, x)).wait_recv()
        mtmp[...] = cbuf[yy, 32:40, :].astype(F32)
        make_block(yy)
        return carry

    lax.fori_loop(1, NY, step, 0)

    stacked = jnp.concatenate([acc[:, 384 * k : 384 * (k + 1)] for k in range(4)], axis=0).T
    rs_send[...] = stacked.astype(BF16).reshape(16, 24, 128)
    sid = c * NZ + z
    rs_out = []
    for d in FAR_FIRST:
        for o in range(NC):
            zz, cc = (z + d) % NZ, (c + o) % NC
            cp = remote(rs_send.at[cc * NZ + zz], rs_recv.at[sid], rs_s.at[d * 2 + o], rs_r.at[sid], (zz, y, cc, x))
            cp.start()
            rs_out.append(cp)
    cp = remote(rs_send.at[(1 - c) * NZ + z], rs_recv.at[sid], rs_s.at[1], rs_r.at[sid], (z, y, 1 - c, x))
    cp.start()
    rs_out.append(cp)

    def wait16(buf, sems, s):
        remote(buf.at[s], buf.at[s], rs_s.at[0], sems.at[s], (z, y, c, x)).wait_recv()

    total = rs_send[sid].astype(F32)
    order16 = [(0, 1)] + [(d, o) for d in NEAR_FIRST for o in range(NC)]
    for d, o in order16:
        s = ((c + o) % NC) * NZ + (z + d) % NZ
        wait16(rs_recv, rs_r, s)
        total = total + rs_recv[s].astype(F32)

    fm = z + c * (y - z)
    sm = y + c * (z - y)

    def at_first(f):
        return (z + (1 - c) * (f - z), y + c * (f - y), c, x)

    def at_second(s):
        return (z + c * (s - z), y + (1 - c) * (s - y), c, x)

    nbuf[sm, fm] = total.astype(BF16)
    g_out = []
    for d in FAR_FIRST:
        ff = (fm + d) % 8
        cp = remote(nbuf.at[sm, fm], nbuf.at[sm, fm], g1_s.at[d], g1_r.at[fm], at_first(ff))
        cp.start()
        g_out.append(cp)
    for d in NEAR_FIRST:
        ff = (fm + d) % 8
        remote(nbuf.at[sm, ff], nbuf.at[sm, ff], g1_s.at[0], g1_r.at[ff], (z, y, c, x)).wait_recv()
    for d in FAR_FIRST:
        ss = (sm + d) % 8
        cp = remote(nbuf.at[sm], nbuf.at[sm], g2_s.at[d], g2_r.at[sm], at_second(ss))
        cp.start()
        g_out.append(cp)

    group = iota((24, 128), 1) >> 5

    def spread_row(s):
        def one(f, carry):
            zz = f + c * (s - f)
            yy = s + c * (f - s)
            n = (zz // 2) * 16 + yy * 2 + zz % 2
            piece = nbuf[s, f].astype(F32)
            for k in range(4):
                wide[n, 24 * k : 24 * (k + 1), :] = jnp.where(group == k, piece, 0.0).astype(BF16)
            return carry

        lax.fori_loop(0, 8, one, 0)

    spread_row(sm)
    for d in NEAR_FIRST:
        ss = (sm + d) % 8
        remote(nbuf.at[ss], nbuf.at[ss], g1_s.at[0], g2_r.at[ss], (z, y, c, x)).wait_recv()
        spread_row(ss)

    for xh in range(2):
        for cs in range(2):
            here = ball.at[xh, pl.ds(96 * cs, 96)]
            mine = (2 * c + xh == x) & (c == cs)

            @pl.when(mine)
            def _():
                own_copy.wait()

            @pl.when(jnp.logical_not(mine))
            def _():
                remote(coupling, here, b_s.at[0], b_r.at[xh * NC + cs], (z, y, c, x)).wait_recv()

    part = jnp.zeros((192, 128), F32)
    for xh in range(2):
        part = part + dot(ball[xh], wide[32 * xh : 32 * (xh + 1)].reshape(3072, 128))
    part = fold(part)
    packs = []
    for r in range(2):
        pack = jnp.zeros((24, 128), F32)
        for k in range(4):
            pack = jnp.where(group == k, part[96 * r + 24 * k : 96 * r + 24 * (k + 1)], pack)
        packs.append(pack)
    xsend[...] = jnp.where(c == 0, packs[1], packs[0])
    xcp = remote(xsend, xrecv, x_s, x_r, (z, y, 1 - c, x))
    xcp.start()
    own = jnp.where(c == 0, packs[0], packs[1])
    xcp.wait()
    qm = 2 * z + c
    mx[qm] = (own + xrecv[...]).astype(BF16)

    e_out = []
    for d in FAR_FIRST:
        for o in range(NC):
            zz, cc = (z + d) % NZ, (c + o) % NC
            cp = remote(mx.at[qm], mx.at[qm], e_s.at[d * 2 + o], e_r.at[qm], (zz, y, cc, x))
            cp.start()
            e_out.append(cp)
    cp = remote(mx.at[qm], mx.at[qm], e_s.at[1], e_r.at[qm], (z, y, 1 - c, x))
    cp.start()
    e_out.append(cp)
    for d, o in order16:
        wait16(mx, e_r, 2 * ((z + d) % NZ) + (c + o) % NC)

    mv = mx[...].astype(F32).reshape(384, 128)
    g384 = iota((384, 128), 1) >> 5
    rhs = jnp.concatenate([jnp.where(g384 == k, mv, 0.0) for k in range(4)], axis=0).astype(BF16)
    g64 = iota((64, 128), 1) >> 5

    def partial(yy):
        full = fold(dot(beta[yy], rhs))
        pack = full[0:64]
        for k in range(1, 4):
            pack = jnp.where(g64 == k, full[64 * k : 64 * (k + 1)], pack)
        return pack

    f_out = []
    for d in FAR_FIRST:
        yy = (y + d) % NY
        fsend[yy] = partial(yy).astype(BF16)
        cp = remote(fsend.at[yy], frecv.at[y], f_s.at[d], f_r.at[y], (z, yy, c, x))
        cp.start()
        f_out.append(cp)
    total = partial(y)
    for d in NEAR_FIRST:
        yy = (y + d) % NY
        remote(frecv.at[yy], frecv.at[yy], f_s.at[0], f_r.at[yy], (z, y, c, x)).wait_recv()
        total = total + frecv[yy].astype(F32)
    for k in range(4):
        out[64 * k : 64 * (k + 1), :] = total[:, 32 * k : 32 * (k + 1)]

    for cp in a_out + b_out + rs_out + g_out + e_out + f_out:
        cp.wait_send()

    @pl.when(side != c)
    def _():
        partner_copy.wait_send()


def shards(coeffs, coupling, miller, species, proj_atom, positions, radial):
    vmem = pl.BlockSpec(memory_space=pltpu.VMEM)
    dma = pltpu.SemaphoreType.DMA
    change = pl.pallas_call(
        kernel,
        out_shape=jax.ShapeDtypeStruct((PW, BANDS), F32),
        in_specs=[vmem] * 6 + [pl.BlockSpec(memory_space=pl.ANY)],
        out_specs=vmem,
        scratch_shapes=[
            pltpu.VMEM((NY, 40, PW), BF16),
            pltpu.VMEM((8, PW), F32),
            pltpu.VMEM((NY, PW, WIDTH), BF16),
            pltpu.VMEM((BANDS, WIDTH), F32),
            pltpu.VMEM((3, 128), F32),
            pltpu.VMEM((128, 128), BF16),
            pltpu.VMEM((128, 128), BF16),
            pltpu.VMEM((128, WIDTH), BF16),
            pltpu.VMEM((256, WIDTH // 2), BF16),
            pltpu.VMEM((8, 128), F32),
            pltpu.VMEM((16, 24, 128), BF16),
            pltpu.VMEM((16, 24, 128), BF16),
            pltpu.VMEM((8, 8, 24, 128), BF16),
            pltpu.VMEM((64, 96, 128), BF16),
            pltpu.VMEM((2, 192, 3072), BF16),
            pltpu.VMEM((24, 128), F32),
            pltpu.VMEM((24, 128), F32),
            pltpu.VMEM((16, 24, 128), BF16),
            pltpu.VMEM((NY, 64, 128), BF16),
            pltpu.VMEM((NY, 64, 128), BF16),
            dma((8,)), dma((8,)), dma((16,)), dma((16,)), dma((8,)), dma((8,)), dma((8,)), dma((8,)),
            dma((4,)), dma((4,)), dma, dma, dma, dma((16,)), dma((16,)), dma((8,)), dma((8,)),
        ],
        compiler_params=pltpu.CompilerParams(
            collective_id=0, has_side_effects=True, vmem_limit_bytes=48 * 1024 * 1024
        ),
    )(
        coeffs, miller, proj_atom.reshape(96, 128), species.reshape(1, ATOMS), positions, radial, coupling
    )
    return (coeffs.astype(F32) + change).astype(BF16)


def solution(mesh):
    torus = Mesh(mesh.devices.reshape(NZ, NY, NC, NX), ("z", "y", "core", "band"))
    return jax.shard_map(
        shards,
        mesh=torus,
        in_specs=(P(GA, "band"), P(GA, "band"), P(None, GA), P(), P(), P(), P()),
        out_specs=P(GA, "band"),
        check_vma=False,
    )
```

```python
import math

import jax
import jax.numpy as jnp
from jax import lax
from jax.experimental import pallas as pl
from jax.experimental.pallas import tpu as pltpu
from jax.sharding import Mesh
from jax.sharding import PartitionSpec as P

NCH = 12
QBINS = 128
MMAX = 24
GA = ("z", "y", "core")
NZ, NY, NC, NX = 8, 8, 2, 4
PW = 256
BANDS = 32
ATOMS = 1024
LANE_ATOMS = 128
ROWS = 64
WIDTH = LANE_ATOMS * NCH
HALF = 6144
SCALE = 1.0 / math.sqrt(32768.0)
MESH = pl.DeviceIdType.MESH
FAR_FIRST = (4, 5, 3, 6, 2, 7, 1)
NEAR_FIRST = (1, 7, 2, 6, 3, 5, 4)
PLACE = {0: 0, 1: 1, 7: 2, 2: 3, 6: 4, 3: 5, 5: 6, 4: 7}
BATCHES = ((0, 5), (5, 8))
F32 = jnp.float32
BF16 = jnp.bfloat16


def dot(a, b, **kw):
    return jnp.dot(a, b, preferred_element_type=F32, **kw)


def split2(v):
    hi = v.astype(BF16)
    return hi, (v - hi.astype(F32)).astype(BF16)


def iota(shape, dim):
    return lax.broadcasted_iota(jnp.int32, shape, dim)


def horner(y, terms):
    acc = jnp.full_like(y, terms[-1])
    for term in terms[-2::-1]:
        acc = acc * y + term
    return acc


SIN_TERMS = (
    3.141592640130705,
    -5.1677100835078935,
    2.5500775232145623,
    -0.5982912856196194,
    0.07765766030331765,
)
COS_TERMS = (
    0.9999999997799042,
    -4.934802137078829,
    4.058709159556242,
    -1.3352120030494103,
    0.2349373138103021,
    -0.024396324339225423,
)


def circle(turns):
    r = turns - jnp.floor(turns + 0.5)
    y = r * r
    s = r * horner(y, SIN_TERMS)
    c = horner(y, COS_TERMS)
    return 1.0 - 2.0 * s * s, 2.0 * s * c


def fold(v):
    v = v + pltpu.roll(v, 32, 1)
    return v + pltpu.roll(v, 64, 1)


def kernel(
    coeffs_h, miller_h, owner_h, species_h, positions_h, radial_h, coupling, out,
    miller, owner, species, positions, radial, in_s, cbuf, mtmp, beta, acc, place, rad3, rad_top, rad_low, perm, back,
    rs_send, rs_recv, nbuf, wide, ball, xsend, xrecv, mx, fsend, frecv,
    a_s, a_r, rs_s, rs_r, g1_s, g1_r, g2_s, g2_r, b_s, b_r, b_l, x_s, x_r, e_s, e_r, f_s, f_r,
):
    z, y, c, x = (lax.axis_index(a) for a in ("z", "y", "core", "band"))
    barrier = pltpu.get_barrier_semaphore()

    loads = [
        pltpu.make_async_copy(src, dst, in_s.at[k])
        for k, (src, dst) in enumerate(
            (
                (miller_h, miller), (coeffs_h, cbuf.at[y, 0:32]), (owner_h, owner),
                (radial_h, radial), (positions_h, positions), (species_h, species),
            )
        )
    ]
    for cp in loads[:2]:
        cp.start()

    def signal(to):
        pl.semaphore_signal(barrier, inc=1, device_id=to, device_id_type=MESH)

    for d in FAR_FIRST:
        signal((z, (y + d) % NY, c, x))
        for o in range(NC):
            signal(((z + d) % NZ, y, (c + o) % NC, x))
    for d in (2, 1, 3):
        for o in range(NC):
            signal((z, y, (c + o) % NC, (x + d) % NX))
    signal((z, y, 1 - c, x))
    greeted = 7 + 14 + 6 + 1

    def remote(src, dst, s, r, to):
        return pltpu.make_async_remote_copy(
            src_ref=src, dst_ref=dst, send_sem=s, recv_sem=r, device_id=to, device_id_type=MESH
        )
    for cp in loads[2:]:
        cp.start()
    for cp in loads[:2]:
        cp.wait()

    mtmp[...] = jnp.zeros_like(mtmp)
    mtmp[0:3, :] = miller[...].astype(F32)
    cbuf[y, 32:40, :] = mtmp[...].astype(BF16)

    pl.semaphore_wait(barrier, greeted)

    a_out = []
    for d in NEAR_FIRST:
        yy = (y + d) % NY
        cp = remote(cbuf.at[y], cbuf.at[y], a_s.at[d], a_r.at[y], (z, yy, c, x))
        cp.start()
        a_out.append(cp)

    side = x // 2

    def half_of(xs, cs, h):
        return ball.at[xs % 2, pl.ds(96 * cs + 48 * h, 48)], 4 * (xs % 2) + 2 * cs + h

    b_out, own_copies, partner_copies = [], [], []
    for first in range(2):
        for way, dx in enumerate((1, 3)):
            h = first if way == 0 else 1 - first
            spot, sem = half_of(x, c, h)
            cp = remote(
                coupling.at[48 * h : 48 * (h + 1)], spot, b_s.at[2 * way + h], b_r.at[sem], (z, y, side, (x + dx) % NX)
            )
            cp.start()
            b_out.append(cp)
    for h in range(2):
        spot, sem = half_of(x, c, h)
        rows = coupling.at[48 * h : 48 * (h + 1)]
        own_copies.append(pltpu.make_async_copy(rows, spot, b_l.at[h]))
        partner_copies.append(remote(rows, spot, b_s.at[4 + h], b_r.at[sem], (z, y, 1 - c, x)))

    @pl.when(side == c)
    def _():
        for cp in own_copies:
            cp.start()

    @pl.when(side != c)
    def _():
        for cp in partner_copies:
            cp.start()

    def moved(natural, ours):
        atom_of = jnp.floor((natural.astype(F32) + 0.5) * (1.0 / NCH)).astype(jnp.int32)
        return (ours == (natural - NCH * atom_of) * 32 + atom_of).astype(F32).astype(BF16)

    square = (384, 384)
    perm[...] = moved(iota(square, 0), iota(square, 1))
    back[...] = moved(iota(square, 1), iota(square, 0))
    acc[...] = jnp.zeros_like(acc)

    for cp in loads[2:]:
        cp.wait()
    col = iota((128, 128), 1)
    j, q, i = col >> 5, (col >> 1) & 15, col & 1
    first = NCH * ((((q >> 1) * NY + y) * NC + (q & 1)) * 8 + j * 2 + i)
    row_of, lane_of = first >> 7, first & 127
    ids = owner[...].astype(F32).T
    ids_hi = jnp.floor(ids * (1.0 / 32.0))
    ids_lo = ids - 32.0 * ids_hi
    pick = (iota((128, 128), 0) == row_of).astype(F32)[0:96, :].astype(BF16)
    at_row = 32.0 * dot(ids_hi.astype(BF16), pick) + dot(ids_lo.astype(BF16), pick)
    atom = jnp.sum(jnp.where(iota((128, 128), 0) == lane_of, at_row, 0.0), axis=0, keepdims=True)
    onehot = (iota((ATOMS, 128), 0) == atom.astype(jnp.int32)).astype(F32)
    place[...] = dot(positions[...], onehot, precision=lax.Precision.HIGHEST)
    kind = dot(species[...].astype(F32).astype(BF16), onehot.astype(BF16))

    rsel = ((iota((128, 12), 0) & 15) == iota((128, 12), 1)).astype(F32)
    rad = dot(rsel, radial[...], precision=lax.Precision.HIGHEST).T * SCALE
    kind3 = 3 * kind.astype(jnp.int32)
    row = iota((128, 128), 0)
    pick_s = jnp.concatenate([(row == kind3 + k).astype(F32) for k in range(3)], axis=1)
    hi, lo = split2(dot(rad, pick_s, precision=lax.Precision.HIGHEST))
    rad_top[0:128, :] = hi
    rad_top[128:256, :] = hi
    rad_low[...] = lo

    def make_block(yy, slot):
        m8 = cbuf[yy, 32:40, :].astype(F32)
        n2 = jnp.sum(m8 * m8, axis=0, keepdims=True)
        qv = n2 * ((QBINS - 1) / (3.0 * MMAX * MMAX))
        mt = jnp.where(iota((8, PW), 0) == 3, qv, m8).T
        hats = jnp.maximum(0.0, 1.0 - jnp.abs(mt[:, 3:4] - iota((PW, 128), 1).astype(F32)))
        h_hi, h_lo = split2(hats)
        rad3[...] = dot(jnp.concatenate([h_hi, h_lo], axis=1), rad_top[...]) + dot(h_hi, rad_low[...])
        for rows in (slice(r, r + ROWS) for r in range(0, PW, ROWS)):
            m0, m1, m2 = (jnp.broadcast_to(mt[rows, k : k + 1], (ROWS, 128)) for k in range(3))
            turns = m0 * place[0:1, :] + m1 * place[1:2, :] + m2 * place[2:3, :]
            cos, sin = circle(turns)
            sin = sin * (1.0 / MMAX)
            phases = (cos, m0 * sin, m1 * sin, m2 * sin)
            for k in range(3):
                amp = rad3[rows, 128 * k : 128 * (k + 1)]
                for t in range(4):
                    ch = 4 * k + t
                    beta[slot, rows, 128 * ch : 128 * (ch + 1)] = (amp * phases[t]).astype(BF16)
        acc[...] += dot(cbuf[yy, 0:32, :], beta[slot])

    make_block(y, 7)

    def step(k, carry):
        d = jnp.where(k % 2 == 1, (k + 1) // 2, NY - k // 2)
        yy = (y + d) % NY
        remote(cbuf.at[yy], cbuf.at[yy], a_s.at[0], a_r.at[yy], (z, y, c, x)).wait_recv()
        make_block(yy, 7 - k)
        return carry

    lax.fori_loop(1, NY, step, 0)

    g32 = iota((32, 128), 1) >> 5

    def lane_tile(j, g):
        tile = jnp.zeros((32, 128), F32)
        for k in range(4):
            chan = acc[:, 128 * (4 * g + k) : 128 * (4 * g + k + 1)]
            if k != j:
                chan = pltpu.roll(chan, (32 * (k - j)) % 128, 1)
            tile = jnp.where(g32 == k, chan, tile)
        return tile

    stacked = jnp.concatenate(
        [jnp.concatenate([lane_tile(j, g) for g in range(3)], axis=1) for j in range(4)], axis=0
    ).T.astype(BF16)
    rs_send[...] = dot(perm[...], stacked).astype(BF16).reshape(16, 24, 128)
    sid = c * NZ + z
    rs_out = []
    for d in FAR_FIRST:
        for o in range(NC):
            zz, cc = (z + d) % NZ, (c + o) % NC
            cp = remote(rs_send.at[cc * NZ + zz], rs_recv.at[sid], rs_s.at[d * 2 + o], rs_r.at[sid], (zz, y, cc, x))
            cp.start()
            rs_out.append(cp)
    cp = remote(rs_send.at[(1 - c) * NZ + z], rs_recv.at[sid], rs_s.at[1], rs_r.at[sid], (z, y, 1 - c, x))
    cp.start()
    rs_out.append(cp)

    near = 2 * c + 1 - x % 2
    which = jnp.where((near + 1) % NX == x, 0, 1)
    for cs in range(2):
        spot, sem = half_of(near, cs, which)
        remote(spot, spot, b_s.at[0], b_r.at[sem], (z, y, c, x)).wait_recv()
        cp = remote(spot, spot, b_s.at[6 + cs], b_r.at[sem], (z, y, c, (near + 2) % NX))
        cp.start()
        b_out.append(cp)

    def wait16(buf, sems, s):
        remote(buf.at[s], buf.at[s], rs_s.at[0], sems.at[s], (z, y, c, x)).wait_recv()

    total = rs_send[sid].astype(F32)
    order16 = [(0, 1)] + [(d, o) for d in NEAR_FIRST for o in range(NC)]
    for d, o in order16:
        s = ((c + o) % NC) * NZ + (z + d) % NZ
        wait16(rs_recv, rs_r, s)
        total = total + rs_recv[s].astype(F32)

    fm = z + c * (y - z)
    sm = y + c * (z - y)

    def at_first(f):
        return (z + (1 - c) * (f - z), y + c * (f - y), c, x)

    def at_second(s):
        return (z + c * (s - z), y + (1 - c) * (s - y), c, x)

    nbuf[sm, 0] = total.astype(BF16)
    g_out = []
    for d in FAR_FIRST:
        k = PLACE[(8 - d) % 8]
        cp = remote(nbuf.at[sm, 0], nbuf.at[sm, k], g1_s.at[d], g1_r.at[k], at_first((fm + d) % 8))
        cp.start()
        g_out.append(cp)
    for batch, (low, high) in enumerate(BATCHES):
        for k in range(max(low, 1), high):
            remote(nbuf.at[sm, k], nbuf.at[sm, k], g1_s.at[0], g1_r.at[k], (z, y, c, x)).wait_recv()
        rows = nbuf.at[sm, low:high]
        for d in FAR_FIRST:
            cp = remote(rows, rows, g2_s.at[batch, d], g2_r.at[batch, sm], at_second((sm + d) % 8))
            cp.start()
            g_out.append(cp)

    group = iota((24, 128), 1) >> 5

    masks = [(group == j).astype(F32).astype(BF16) for j in range(4)]

    def spread_rows(s, low, high):
        for k in range(low, high):
            f = (fm + ((k + 1) // 2 if k % 2 else 8 - k // 2)) % 8
            zz = f + c * (s - f)
            yy = s + c * (f - s)
            n = (zz // 2) * 16 + yy * 2 + zz % 2
            piece = nbuf[s, k]
            for j in range(4):
                wide[n, 24 * j : 24 * (j + 1), :] = piece * masks[j]

    spread_rows(sm, 0, 8)
    for batch, (low, high) in enumerate(BATCHES):
        for d in NEAR_FIRST:
            ss = (sm + d) % 8
            rows = nbuf.at[ss, low:high]
            remote(rows, rows, g1_s.at[0], g2_r.at[batch, ss], (z, y, c, x)).wait_recv()
            spread_rows(ss, low, high)

    for xh in range(2):
        for cs in range(2):
            for h in range(2):
                xs = 2 * c + xh
                mine = (xs == x) & (c == cs)
                passed = (xs == near) & (which == h)
                spot, sem = half_of(xs, cs, h)

                @pl.when(mine)
                def _():
                    own_copies[h].wait()

                @pl.when(jnp.logical_not(mine | passed))
                def _():
                    remote(spot, spot, b_s.at[0], b_r.at[sem], (z, y, c, x)).wait_recv()

    part = jnp.zeros((192, 128), F32)
    for xh in range(2):
        part = part + dot(ball[xh], wide[32 * xh : 32 * (xh + 1)].reshape(3072, 128))
    part = fold(part)
    packs = []
    for r in range(2):
        pack = jnp.zeros((24, 128), F32)
        for k in range(4):
            pack = jnp.where(group == k, part[96 * r + 24 * k : 96 * r + 24 * (k + 1)], pack)
        packs.append(pack)
    xsend[...] = jnp.where(c == 0, packs[1], packs[0])
    xcp = remote(xsend, xrecv, x_s, x_r, (z, y, 1 - c, x))
    xcp.start()
    own = jnp.where(c == 0, packs[0], packs[1])
    xcp.wait()
    qm = 2 * z + c
    mx[qm] = (own + xrecv[...]).astype(BF16)

    e_out = []
    for d in FAR_FIRST:
        for o in range(NC):
            zz, cc = (z + d) % NZ, (c + o) % NC
            cp = remote(mx.at[qm], mx.at[qm], e_s.at[d * 2 + o], e_r.at[qm], (zz, y, cc, x))
            cp.start()
            e_out.append(cp)
    cp = remote(mx.at[qm], mx.at[qm], e_s.at[1], e_r.at[qm], (z, y, 1 - c, x))
    cp.start()
    e_out.append(cp)
    for d, o in order16:
        wait16(mx, e_r, 2 * ((z + d) % NZ) + (c + o) % NC)

    ours = dot(back[...], mx[...].reshape(384, 128))
    ours = ours.T

    def channel(k):
        tile = jnp.zeros((32, 128), F32)
        for j in range(4):
            part = ours[32 * j : 32 * (j + 1), 128 * (k // 4) : 128 * (k // 4 + 1)]
            if k % 4 != j:
                part = pltpu.roll(part, (32 * (j - k % 4)) % 128, 1)
            tile = jnp.where(g32 == j, part, tile)
        return tile

    lhs = jnp.concatenate([channel(k) for k in range(NCH)], axis=1).astype(BF16)

    f_out = []
    for pair in range(4):
        both = lax.dot_general(
            lhs, beta[2 * pair : 2 * pair + 2].reshape(2 * PW, WIDTH),
            (((1,), (1,)), ((), ())), preferred_element_type=F32,
        )
        for half in range(2):
            total = both[:, PW * half : PW * (half + 1)]
            slot = 2 * pair + half
            if slot == 7:
                break
            d = FAR_FIRST[slot]
            yy = (y + d) % NY
            fsend[slot] = total.astype(BF16)
            cp = remote(fsend.at[slot], frecv.at[y], f_s.at[d], f_r.at[y], (z, yy, c, x))
            cp.start()
            f_out.append(cp)
    for d in NEAR_FIRST:
        yy = (y + d) % NY
        remote(frecv.at[yy], frecv.at[yy], f_s.at[0], f_r.at[yy], (z, y, c, x)).wait_recv()
        total = total + frecv[yy].astype(F32)
    out[...] = total

    for cp in a_out + b_out + rs_out + g_out + e_out + f_out:
        cp.wait_send()

    @pl.when(side != c)
    def _():
        for cp in partner_copies:
            cp.wait_send()


def shards(coeffs, coupling, miller, species, proj_atom, positions, radial):
    vmem = pl.BlockSpec(memory_space=pltpu.VMEM)
    dma = pltpu.SemaphoreType.DMA
    change = pl.pallas_call(
        kernel,
        out_shape=jax.ShapeDtypeStruct((BANDS, PW), F32),
        in_specs=[pl.BlockSpec(memory_space=pl.ANY)] * 7,
        out_specs=vmem,
        scratch_shapes=[
            pltpu.VMEM((3, PW), jnp.int32),
            pltpu.VMEM((96, 128), jnp.int32),
            pltpu.VMEM((1, ATOMS), jnp.int32),
            pltpu.VMEM((3, ATOMS), F32),
            pltpu.VMEM((12, QBINS), F32),
            dma((6,)),
            pltpu.VMEM((NY, 40, PW), BF16),
            pltpu.VMEM((8, PW), F32),
            pltpu.VMEM((NY, PW, WIDTH), BF16),
            pltpu.VMEM((BANDS, WIDTH), F32),
            pltpu.VMEM((3, 128), F32),
            pltpu.VMEM((PW, 384), F32),
            pltpu.VMEM((256, 384), BF16),
            pltpu.VMEM((128, 384), BF16),
            pltpu.VMEM((384, 384), BF16),
            pltpu.VMEM((384, 384), BF16),
            pltpu.VMEM((16, 24, 128), BF16),
            pltpu.VMEM((16, 24, 128), BF16),
            pltpu.VMEM((8, 8, 24, 128), BF16),
            pltpu.VMEM((64, 96, 128), BF16),
            pltpu.VMEM((2, 192, 3072), BF16),
            pltpu.VMEM((24, 128), F32),
            pltpu.VMEM((24, 128), F32),
            pltpu.VMEM((16, 24, 128), BF16),
            pltpu.VMEM((NY, BANDS, PW), BF16),
            pltpu.VMEM((NY, BANDS, PW), BF16),
            dma((8,)), dma((8,)), dma((16,)), dma((16,)), dma((8,)), dma((8,)), dma((2, 8)), dma((2, 8)),
            dma((8,)), dma((8,)), dma((2,)), dma, dma, dma((16,)), dma((16,)), dma((8,)), dma((8,)),
        ],
        compiler_params=pltpu.CompilerParams(
            collective_id=0, has_side_effects=True, vmem_limit_bytes=67043328 - 65536
        ),
    )(
        coeffs.T, miller, proj_atom.reshape(96, 128), species.reshape(1, ATOMS), positions, radial, coupling
    )
    return (coeffs.T.astype(F32) + change).astype(BF16).T


def solution(mesh):
    torus = Mesh(mesh.devices.reshape(NZ, NY, NC, NX), ("z", "y", "core", "band"))
    return jax.shard_map(
        shards,
        mesh=torus,
        in_specs=(P(GA, "band"), P(GA, "band"), P(None, GA), P(), P(), P(), P()),
        out_specs=P(GA, "band"),
        check_vma=False,
    )
```

```python
import math

import jax
import jax.numpy as jnp
from jax import lax
from jax.experimental import pallas as pl
from jax.experimental.pallas import tpu as pltpu
from jax.sharding import Mesh
from jax.sharding import PartitionSpec as P

NCH = 12
QBINS = 128
MMAX = 24
GA = ("z", "y", "core")
NZ, NY, NC, NX = 8, 8, 2, 4
PW = 256
BANDS = 32
ATOMS = 1024
LANE_ATOMS = 128
ROWS = 64
WIDTH = LANE_ATOMS * NCH
HALF = 6144
SCALE = 1.0 / math.sqrt(32768.0)
MESH = pl.DeviceIdType.MESH
FAR_FIRST = (4, 5, 3, 6, 2, 7, 1)
NEAR_FIRST = (1, 7, 2, 6, 3, 5, 4)
PLACE = {0: 0, 1: 1, 7: 2, 2: 3, 6: 4, 3: 5, 5: 6, 4: 7}
BATCHES = ((0, 1), (1, 3), (3, 5), (5, 8))
BATCH_OF = (0, 1, 1, 2, 2, 3, 3, 3)
F32 = jnp.float32
BF16 = jnp.bfloat16


def dot(a, b, **kw):
    return jnp.dot(a, b, preferred_element_type=F32, **kw)


def split2(v):
    hi = v.astype(BF16)
    return hi, (v - hi.astype(F32)).astype(BF16)


def iota(shape, dim):
    return lax.broadcasted_iota(jnp.int32, shape, dim)


def horner(y, terms):
    acc = jnp.full_like(y, terms[-1])
    for term in terms[-2::-1]:
        acc = acc * y + term
    return acc


SIN_TERMS = (
    3.141590270206989,
    -5.167406733272336,
    2.544010518503403,
    -0.5594624554679108,
)
COS_TERMS = (
    0.9999999532476079,
    -4.934792830619647,
    4.058411352862676,
    -1.3318765680812747,
    0.21968961109860236,
)


def circle(turns):
    r = turns - jnp.floor(turns + 0.5)
    y = r * r
    s = r * horner(y, SIN_TERMS)
    return 1.0 - 2.0 * (s * s), s * (horner(y, [t * (2.0 / MMAX) for t in COS_TERMS]))


def fold(v):
    v = v + pltpu.roll(v, 32, 1)
    return v + pltpu.roll(v, 64, 1)


def kernel(
    coeffs_h, miller_h, owner_h, species_h, positions_h, radial_h, coupling, out,
    miller, owner, species, positions, radial, in_s, cbuf, mtmp, beta, acc, place, rad3, rad_top, rad_low, perm, back,
    rs_send, rs_recv, nbuf, wide, ball, xsend, xrecv, mx, fsend, frecv,
    a_s, a_r, rs_s, rs_r, g1_s, g1_r, g2_s, g2_r, b_s, b_r, b_l, x_s, x_r, e_s, e_r, f_s, f_r,
):
    z, y, c, x = (lax.axis_index(a) for a in ("z", "y", "core", "band"))
    barrier = pltpu.get_barrier_semaphore()

    loads = [
        pltpu.make_async_copy(src, dst, in_s.at[k])
        for k, (src, dst) in enumerate(
            (
                (miller_h, miller), (coeffs_h, cbuf.at[y, 0:32]), (owner_h, owner),
                (radial_h, radial), (positions_h, positions), (species_h, species),
            )
        )
    ]
    for cp in loads[:2]:
        cp.start()

    def signal(to):
        pl.semaphore_signal(barrier, inc=1, device_id=to, device_id_type=MESH)

    for d in FAR_FIRST:
        signal((z, (y + d) % NY, c, x))
        for o in range(NC):
            signal(((z + d) % NZ, y, (c + o) % NC, x))
    for d in (2, 1, 3):
        for o in range(NC):
            signal((z, y, (c + o) % NC, (x + d) % NX))
    signal((z, y, 1 - c, x))
    greeted = 7 + 14 + 6 + 1

    def remote(src, dst, s, r, to):
        return pltpu.make_async_remote_copy(
            src_ref=src, dst_ref=dst, send_sem=s, recv_sem=r, device_id=to, device_id_type=MESH
        )
    for cp in loads[2:]:
        cp.start()
    for cp in loads[:2]:
        cp.wait()

    mtmp[...] = jnp.zeros_like(mtmp)
    mtmp[0:3, :] = miller[...].astype(F32)
    cbuf[y, 32:40, :] = mtmp[...].astype(BF16)

    def moved(natural, ours):
        atom_of = jnp.floor((natural.astype(F32) + 0.5) * (1.0 / NCH)).astype(jnp.int32)
        return (ours == (natural - NCH * atom_of) * 32 + atom_of).astype(F32).astype(BF16)

    square = (384, 384)
    perm[...] = moved(iota(square, 0), iota(square, 1))
    back[...] = moved(iota(square, 1), iota(square, 0))
    acc[...] = jnp.zeros_like(acc)

    for cp in loads[2:]:
        cp.wait()
    col = iota((128, 128), 1)
    j, q, i = col >> 5, (col >> 1) & 15, col & 1
    first = NCH * ((((q >> 1) * NY + y) * NC + (q & 1)) * 8 + j * 2 + i)
    row_of, lane_of = first >> 7, first & 127
    ids = owner[...].astype(F32).T
    ids_hi = jnp.floor(ids * (1.0 / 32.0))
    ids_lo = ids - 32.0 * ids_hi
    pick = (iota((128, 128), 0) == row_of).astype(F32)[0:96, :].astype(BF16)
    at_row = 32.0 * dot(ids_hi.astype(BF16), pick) + dot(ids_lo.astype(BF16), pick)
    atom = jnp.sum(jnp.where(iota((128, 128), 0) == lane_of, at_row, 0.0), axis=0, keepdims=True)
    onehot = (iota((ATOMS, 128), 0) == atom.astype(jnp.int32)).astype(F32)
    place[...] = dot(positions[...], onehot, precision=lax.Precision.HIGHEST)
    kind = dot(species[...].astype(F32).astype(BF16), onehot.astype(BF16))

    rsel = ((iota((128, 12), 0) & 15) == iota((128, 12), 1)).astype(F32)
    rad = dot(rsel, radial[...], precision=lax.Precision.HIGHEST).T * SCALE
    kind3 = 3 * kind.astype(jnp.int32)
    row = iota((128, 128), 0)
    pick_s = jnp.concatenate([(row == kind3 + k).astype(F32) for k in range(3)], axis=1)
    hi, lo = split2(dot(rad, pick_s, precision=lax.Precision.HIGHEST))
    rad_top[0:128, :] = hi
    rad_top[128:256, :] = hi
    rad_low[...] = lo

    pl.semaphore_wait(barrier, greeted)

    for d in NEAR_FIRST:
        yy = (y + d) % NY
        remote(cbuf.at[y], cbuf.at[y], a_s, a_r.at[y], (z, yy, c, x)).start()

    side = x // 2

    def half_of(xs, cs, h):
        return ball.at[xs % 2, pl.ds(96 * cs + 48 * h, 48)], 4 * (xs % 2) + 2 * cs + h

    own_copies, partner_copies = [], []
    for first in range(2):
        for way, dx in enumerate((1, 3)):
            h = first if way == 0 else 1 - first
            spot, sem = half_of(x, c, h)
            cp = remote(
                coupling.at[48 * h : 48 * (h + 1)], spot, b_s.at[0], b_r.at[sem], (z, y, side, (x + dx) % NX)
            )
            cp.start()
    for h in range(2):
        spot, sem = half_of(x, c, h)
        rows = coupling.at[48 * h : 48 * (h + 1)]
        own_copies.append(pltpu.make_async_copy(rows, spot, b_l.at[h]))
        partner_copies.append(remote(rows, spot, b_s.at[1], b_r.at[sem], (z, y, 1 - c, x)))

    @pl.when(side == c)
    def _():
        for cp in own_copies:
            cp.start()

    @pl.when(side != c)
    def _():
        for cp in partner_copies:
            cp.start()

    def make_block(yy, slot):
        m8 = cbuf[yy, 32:40, :].astype(F32)
        n2 = jnp.sum(m8 * m8, axis=0, keepdims=True)
        qv = n2 * ((QBINS - 1) / (3.0 * MMAX * MMAX))
        mt = jnp.where(iota((8, PW), 0) == 3, qv, m8).T
        hats = jnp.maximum(0.0, 1.0 - jnp.abs(mt[:, 3:4] - iota((PW, 128), 1).astype(F32)))
        h_hi, h_lo = split2(hats)
        rad3[...] = dot(jnp.concatenate([h_hi, h_lo], axis=1), rad_top[...]) + dot(h_hi, rad_low[...])
        for rows in (slice(r, r + ROWS) for r in range(0, PW, ROWS)):
            m0, m1, m2 = (jnp.broadcast_to(mt[rows, k : k + 1], (ROWS, 128)) for k in range(3))
            turns = m0 * place[0:1, :] + m1 * place[1:2, :] + m2 * place[2:3, :]
            cos, sin = circle(turns)
            phases = (cos, m0 * sin, m1 * sin, m2 * sin)
            for k in range(3):
                amp = rad3[rows, 128 * k : 128 * (k + 1)]
                for t in range(4):
                    ch = 4 * k + t
                    beta[slot, rows, 128 * ch : 128 * (ch + 1)] = (amp * phases[t]).astype(BF16)

    def project(yy, slot):
        acc[...] += dot(cbuf[yy, 0:32, :], beta[slot])

    make_block(y, 7)

    last = (y, 7)
    for k, d in enumerate(NEAR_FIRST):
        yy = (y + d) % NY
        remote(cbuf.at[yy], cbuf.at[yy], a_s, a_r.at[yy], (z, y, c, x)).wait_recv()
        project(*last)
        last = (yy, 6 - k)
        make_block(*last)
    project(*last)

    g32 = iota((32, 128), 1) >> 5

    def lane_tile(j, g):
        tile = jnp.zeros((32, 128), F32)
        for k in range(4):
            chan = acc[:, 128 * (4 * g + k) : 128 * (4 * g + k + 1)]
            if k != j:
                chan = pltpu.roll(chan, (32 * (k - j)) % 128, 1)
            tile = jnp.where(g32 == k, chan, tile)
        return tile

    stacked = jnp.concatenate(
        [jnp.concatenate([lane_tile(j, g) for g in range(3)], axis=1) for j in range(4)], axis=0
    ).T.astype(BF16)
    rs_send[...] = dot(perm[...], stacked).astype(BF16).reshape(16, 24, 128)
    sid = c * NZ + z
    for d in FAR_FIRST:
        for o in range(NC):
            zz, cc = (z + d) % NZ, (c + o) % NC
            remote(rs_send.at[cc * NZ + zz], rs_recv.at[sid], rs_s, rs_r, (zz, y, cc, x)).start()
    remote(rs_send.at[(1 - c) * NZ + z], rs_recv.at[sid], rs_s, rs_r, (z, y, 1 - c, x)).start()

    near = 2 * c + 1 - x % 2
    which = jnp.where((near + 1) % NX == x, 0, 1)
    for cs in range(2):
        spot, sem = half_of(near, cs, which)
        remote(spot, spot, b_s.at[0], b_r.at[sem], (z, y, c, x)).wait_recv()
        remote(spot, spot, b_s.at[2], b_r.at[sem], (z, y, c, (near + 2) % NX)).start()

    def received(buf, sem):
        remote(buf, buf, rs_s, sem, (z, y, c, x)).wait_recv()

    def sent(buf, sem):
        remote(buf, buf, sem, rs_r, (z, y, c, x)).wait_send()

    received(rs_recv.at[0:15], rs_r)
    total = rs_send[sid].astype(F32)
    for d in range(NZ):
        for o in range(NC):
            if d or o:
                total = total + rs_recv[((c + o) % NC) * NZ + (z + d) % NZ].astype(F32)

    fm = z + c * (y - z)
    sm = y + c * (z - y)

    def at_first(f):
        return (z + (1 - c) * (f - z), y + c * (f - y), c, x)

    def at_second(s):
        return (z + c * (s - z), y + (1 - c) * (s - y), c, x)

    nbuf[sm, 0] = total.astype(BF16)
    for d in FAR_FIRST:
        k = PLACE[(8 - d) % 8]
        remote(nbuf.at[sm, 0], nbuf.at[sm, k], g1_s, g1_r.at[BATCH_OF[k]], at_first((fm + d) % 8)).start()
    for batch, (low, high) in enumerate(BATCHES):
        if batch:
            received(nbuf.at[sm, low:high], g1_r.at[batch])
        rows = nbuf.at[sm, low:high]
        for d in FAR_FIRST:
            remote(rows, rows, g2_s, g2_r.at[sm], at_second((sm + d) % 8)).start()

    group = iota((24, 128), 1) >> 5

    masks = [(group == j).astype(F32).astype(BF16) for j in range(4)]

    def spread_row(s):
        for k in range(8):
            f = (fm + ((k + 1) // 2 if k % 2 else 8 - k // 2)) % 8
            zz = f + c * (s - f)
            yy = s + c * (f - s)
            n = (zz // 2) * 16 + yy * 2 + zz % 2
            piece = nbuf[s, k]
            for j in range(4):
                wide[n, 24 * j : 24 * (j + 1), :] = piece * masks[j]

    spread_row(sm)
    for d in NEAR_FIRST:
        ss = (sm + d) % 8
        received(nbuf.at[ss], g2_r.at[ss])
        spread_row(ss)

    for xh in range(2):
        for cs in range(2):
            for h in range(2):
                xs = 2 * c + xh
                mine = (xs == x) & (c == cs)
                passed = (xs == near) & (which == h)
                spot, sem = half_of(xs, cs, h)

                @pl.when(mine)
                def _():
                    own_copies[h].wait()

                @pl.when(jnp.logical_not(mine | passed))
                def _():
                    remote(spot, spot, b_s.at[0], b_r.at[sem], (z, y, c, x)).wait_recv()

    def product(r):
        rows = pl.ds(pl.multiple_of(96 * r, 32), 96)
        part = jnp.zeros((96, 128), F32)
        for xh in range(2):
            part = part + dot(ball[xh, rows], wide[32 * xh : 32 * (xh + 1)].reshape(3072, 128))
        part = fold(part)
        pack = part[0:24]
        for k in range(1, 4):
            pack = jnp.where(group == k, part[24 * k : 24 * (k + 1)], pack)
        return pack

    xsend[...] = product(1 - c)
    xcp = remote(xsend, xrecv, x_s, x_r, (z, y, 1 - c, x))
    xcp.start()
    own = product(c)
    xcp.wait()
    qm = 2 * z + c
    mx[qm] = (own + xrecv[...]).astype(BF16)

    for d in FAR_FIRST:
        for o in range(NC):
            zz, cc = (z + d) % NZ, (c + o) % NC
            remote(mx.at[qm], mx.at[qm], e_s, e_r, (zz, y, cc, x)).start()
    remote(mx.at[qm], mx.at[qm], e_s, e_r, (z, y, 1 - c, x)).start()
    received(mx.at[0:15], e_r)

    ours = dot(back[...], mx[...].reshape(384, 128))
    ours = ours.T

    def channel(k):
        tile = jnp.zeros((32, 128), F32)
        for j in range(4):
            part = ours[32 * j : 32 * (j + 1), 128 * (k // 4) : 128 * (k // 4 + 1)]
            if k % 4 != j:
                part = pltpu.roll(part, (32 * (j - k % 4)) % 128, 1)
            tile = jnp.where(g32 == j, part, tile)
        return tile

    lhs = jnp.concatenate([channel(k) for k in range(NCH)], axis=1).astype(BF16)

    for pair in range(4):
        both = lax.dot_general(
            lhs, beta[2 * pair : 2 * pair + 2].reshape(2 * PW, WIDTH),
            (((1,), (1,)), ((), ())), preferred_element_type=F32,
        )
        for half in range(2):
            total = both[:, PW * half : PW * (half + 1)]
            slot = 2 * pair + half
            if slot == 7:
                break
            d = FAR_FIRST[slot]
            yy = (y + d) % NY
            fsend[slot] = total.astype(BF16)
            remote(fsend.at[slot], frecv.at[y], f_s, f_r, (z, yy, c, x)).start()
    received(frecv.at[0:7], f_r)
    for d in NEAR_FIRST:
        total = total + frecv[(y + d) % NY].astype(F32)
    out[...] = total

    sent(cbuf.at[0:7], a_s)
    sent(ball.at[0], b_s.at[0])
    sent(ball.at[0, 0:96], b_s.at[2])
    sent(rs_send.at[0:15], rs_s)
    sent(nbuf.at[0, 0:7], g1_s)
    sent(nbuf.at[0:7], g2_s)
    sent(mx.at[0:15], e_s)
    sent(fsend.at[0:7], f_s)

    @pl.when(side != c)
    def _():
        sent(ball.at[0, 0:96], b_s.at[1])


def shards(coeffs, coupling, miller, species, proj_atom, positions, radial):
    vmem = pl.BlockSpec(memory_space=pltpu.VMEM)
    dma = pltpu.SemaphoreType.DMA
    inputs = (
        coeffs.T, miller, proj_atom.reshape(96, 128), species.reshape(1, ATOMS), positions, radial, coupling
    )
    change = pl.pallas_call(
        kernel,
        out_shape=jax.ShapeDtypeStruct((BANDS, PW), F32),
        in_specs=[pl.BlockSpec(memory_space=pl.ANY)] * 7,
        out_specs=vmem,
        scratch_shapes=[
            pltpu.VMEM((3, PW), jnp.int32),
            pltpu.VMEM((96, 128), jnp.int32),
            pltpu.VMEM((1, ATOMS), jnp.int32),
            pltpu.VMEM((3, ATOMS), F32),
            pltpu.VMEM((12, QBINS), F32),
            dma((6,)),
            pltpu.VMEM((NY, 40, PW), BF16),
            pltpu.VMEM((8, PW), F32),
            pltpu.VMEM((NY, PW, WIDTH), BF16),
            pltpu.VMEM((BANDS, WIDTH), F32),
            pltpu.VMEM((3, 128), F32),
            pltpu.VMEM((PW, 384), F32),
            pltpu.VMEM((256, 384), BF16),
            pltpu.VMEM((128, 384), BF16),
            pltpu.VMEM((384, 384), BF16),
            pltpu.VMEM((384, 384), BF16),
            pltpu.VMEM((16, 24, 128), BF16),
            pltpu.VMEM((16, 24, 128), BF16),
            pltpu.VMEM((8, 8, 24, 128), BF16),
            pltpu.VMEM((64, 96, 128), BF16),
            pltpu.VMEM((2, 192, 3072), BF16),
            pltpu.VMEM((24, 128), F32),
            pltpu.VMEM((24, 128), F32),
            pltpu.VMEM((16, 24, 128), BF16),
            pltpu.VMEM((NY, BANDS, PW), BF16),
            pltpu.VMEM((NY, BANDS, PW), BF16),
            dma, dma((8,)), dma, dma, dma, dma((4,)), dma, dma((8,)),
            dma((3,)), dma((8,)), dma((2,)), dma, dma, dma, dma, dma, dma,
        ],
        compiler_params=pltpu.CompilerParams(
            collective_id=0, has_side_effects=True, vmem_limit_bytes=48 * 1024 * 1024
        ),
    )(
        *(pltpu.with_memory_space_constraint(v, pltpu.HBM) for v in inputs)
    )
    return (coeffs.T.astype(F32) + change).astype(BF16).T


def solution(mesh):
    torus = Mesh(mesh.devices.reshape(NZ, NY, NC, NX), ("z", "y", "core", "band"))
    return jax.shard_map(
        shards,
        mesh=torus,
        in_specs=(P(GA, "band"), P(GA, "band"), P(None, GA), P(), P(), P(), P()),
        out_specs=P(GA, "band"),
        check_vma=False,
    )
```

```python
import math

import jax
import jax.numpy as jnp
from jax import lax
from jax.experimental import pallas as pl
from jax.experimental.pallas import tpu as pltpu
from jax.sharding import Mesh
from jax.sharding import PartitionSpec as P

NCH = 12
QBINS = 128
MMAX = 24
GA = ("z", "y", "core")
NZ, NY, NC, NX = 8, 8, 2, 4
PW = 256
BANDS = 32
ATOMS = 1024
LANE_ATOMS = 128
ROWS = 64
WIDTH = LANE_ATOMS * NCH
HALF = 6144
SCALE = 1.0 / math.sqrt(32768.0)
MESH = pl.DeviceIdType.MESH
LAG = 2
GROUPS = ((0, 1), (1, 2), (2, 4), (4, 6), (6, 8))
FAR_FIRST = (4, 5, 3, 6, 2, 7, 1)
NEAR_FIRST = (1, 7, 2, 6, 3, 5, 4)
PLACE = {0: 0, 1: 1, 7: 2, 2: 3, 6: 4, 3: 5, 5: 6, 4: 7}
BATCHES = ((0, 1), (1, 3), (3, 5), (5, 8))
BATCH_OF = (0, 1, 1, 2, 2, 3, 3, 3)
F32 = jnp.float32
BF16 = jnp.bfloat16


def dot(a, b, **kw):
    return jnp.dot(a, b, preferred_element_type=F32, **kw)


def split2(v):
    hi = v.astype(BF16)
    return hi, (v - hi.astype(F32)).astype(BF16)


def iota(shape, dim):
    return lax.broadcasted_iota(jnp.int32, shape, dim)


def horner(y, terms):
    acc = jnp.full_like(y, terms[-1])
    for term in terms[-2::-1]:
        acc = acc * y + term
    return acc


SIN_TERMS = (
    3.141590270206989,
    -5.167406733272336,
    2.544010518503403,
    -0.5594624554679108,
)
COS_TERMS = (
    0.9999999532476079,
    -4.934792830619647,
    4.058411352862676,
    -1.3318765680812747,
    0.21968961109860236,
)


def circle(turns):
    r = turns - jnp.floor(turns + 0.5)
    y = r * r
    s = r * horner(y, SIN_TERMS)
    return 1.0 - 2.0 * (s * s), s * (horner(y, [t * (2.0 / MMAX) for t in COS_TERMS]))


def fold(v):
    v = v + pltpu.roll(v, 32, 1)
    return v + pltpu.roll(v, 64, 1)


def kernel(
    coeffs_h, miller_h, owner_h, species_h, positions_h, radial_h, coupling, out,
    miller, owner, species, positions, radial, in_s, cbuf, mbuf, mtmp, beta, acc, place, rad3, rad_top, perm, back,
    rs_send, rs_recv, nbuf, wide, ball, xsend, xrecv, mx, fsend, frecv,
    m_s, m_r, a_s, a_r, rs_s, rs_r, g1_s, g1_r, g2_s, g2_r, b_s, b_r, b_l, x_s, x_r, e_s, e_r, f_s, f_r,
):
    z, y, c, x = (lax.axis_index(a) for a in ("z", "y", "core", "band"))
    barrier = pltpu.get_barrier_semaphore()

    loads = [
        pltpu.make_async_copy(src, dst, in_s.at[k])
        for k, (src, dst) in enumerate(
            (
                (miller_h, miller), (coeffs_h, cbuf.at[y]), (owner_h, owner),
                (radial_h, radial), (positions_h, positions), (species_h, species),
            )
        )
    ]
    for cp in loads[:2]:
        cp.start()

    def signal(to):
        pl.semaphore_signal(barrier, inc=1, device_id=to, device_id_type=MESH)

    for d in FAR_FIRST:
        signal((z, (y + d) % NY, c, x))
        for o in range(NC):
            signal(((z + d) % NZ, y, (c + o) % NC, x))
    for d in (2, 1, 3):
        for o in range(NC):
            signal((z, y, (c + o) % NC, (x + d) % NX))
    signal((z, y, 1 - c, x))
    greeted = 7 + 14 + 6 + 1

    def remote(src, dst, s, r, to):
        return pltpu.make_async_remote_copy(
            src_ref=src, dst_ref=dst, send_sem=s, recv_sem=r, device_id=to, device_id_type=MESH
        )
    for cp in loads[2:]:
        cp.start()
    def moved(natural, ours):
        atom_of = jnp.floor((natural.astype(F32) + 0.5) * (1.0 / NCH)).astype(jnp.int32)
        return (ours == (natural - NCH * atom_of) * 32 + atom_of).astype(F32).astype(BF16)

    square = (384, 384)
    perm[...] = moved(iota(square, 0), iota(square, 1))
    back[...] = moved(iota(square, 1), iota(square, 0))
    acc[...] = jnp.zeros_like(acc)

    for cp in loads[:2]:
        cp.wait()

    mtmp[...] = jnp.zeros_like(mtmp)
    mtmp[0:3, :] = miller[...].astype(F32)
    mbuf[y] = mtmp[...].astype(BF16)

    for cp in loads[2:]:
        cp.wait()
    col = iota((128, 128), 1)
    j, q, i = col >> 5, (col >> 1) & 15, col & 1
    first = NCH * ((((q >> 1) * NY + y) * NC + (q & 1)) * 8 + j * 2 + i)
    row_of, lane_of = first >> 7, first & 127
    ids = owner[...].astype(F32).T
    ids_hi = jnp.floor(ids * (1.0 / 32.0))
    ids_lo = ids - 32.0 * ids_hi
    pick = (iota((128, 128), 0) == row_of).astype(F32)[0:96, :].astype(BF16)
    at_row = 32.0 * dot(ids_hi.astype(BF16), pick) + dot(ids_lo.astype(BF16), pick)
    atom = jnp.sum(jnp.where(iota((128, 128), 0) == lane_of, at_row, 0.0), axis=0, keepdims=True)
    onehot = (iota((ATOMS, 128), 0) == atom.astype(jnp.int32)).astype(F32)
    place[...] = dot(positions[...], onehot, precision=lax.Precision.HIGHEST)
    kind = dot(species[...].astype(F32).astype(BF16), onehot.astype(BF16))

    rsel = ((iota((128, 12), 0) & 15) == iota((128, 12), 1)).astype(F32)
    rad = dot(rsel, radial[...], precision=lax.Precision.HIGHEST).T * SCALE
    kind3 = 3 * kind.astype(jnp.int32)
    row = iota((128, 128), 0)
    pick_s = jnp.concatenate([(row == kind3 + k).astype(F32) for k in range(3)], axis=1)
    hi, lo = split2(dot(rad, pick_s, precision=lax.Precision.HIGHEST))
    rad_top[0:128, :] = hi
    rad_top[128:256, :] = hi
    rad_top[256:384, :] = lo

    pl.semaphore_wait(barrier, greeted)

    for d in NEAR_FIRST:
        remote(mbuf.at[y], mbuf.at[y], m_s, m_r.at[y], (z, (y + d) % NY, c, x)).start()
    for d in NEAR_FIRST:
        yy = (y + d) % NY
        remote(cbuf.at[y], cbuf.at[y], a_s, a_r.at[y], (z, yy, c, x)).start()

    side = x // 2

    def half_of(xs, cs, h):
        return ball.at[xs % 2, pl.ds(96 * cs + 48 * h, 48)], 4 * (xs % 2) + 2 * cs + h

    own_copies, partner_copies = [], []
    for first in range(2):
        for way, dx in enumerate((1, 3)):
            h = first if way == 0 else 1 - first
            spot, sem = half_of(x, c, h)
            cp = remote(
                coupling.at[48 * h : 48 * (h + 1)], spot, b_s.at[0], b_r.at[sem], (z, y, side, (x + dx) % NX)
            )
            cp.start()
    for h in range(2):
        spot, sem = half_of(x, c, h)
        rows = coupling.at[48 * h : 48 * (h + 1)]
        own_copies.append(pltpu.make_async_copy(rows, spot, b_l.at[h]))
        partner_copies.append(remote(rows, spot, b_s.at[1], b_r.at[sem], (z, y, 1 - c, x)))

    @pl.when(side == c)
    def _():
        for cp in own_copies:
            cp.start()

    @pl.when(side != c)
    def _():
        for cp in partner_copies:
            cp.start()

    def make_block(yy, slot):
        m8 = mbuf[yy].astype(F32)
        n2 = jnp.sum(m8 * m8, axis=0, keepdims=True)
        qv = n2 * ((QBINS - 1) / (3.0 * MMAX * MMAX))
        mt = jnp.where(iota((8, PW), 0) == 3, qv, m8).T
        hats = jnp.maximum(0.0, 1.0 - jnp.abs(mt[:, 3:4] - iota((PW, 128), 1).astype(F32)))
        h_hi, h_lo = split2(hats)
        rad3[...] = dot(jnp.concatenate([h_hi, h_lo, h_hi], axis=1), rad_top[...])
        for rows in (slice(r, r + ROWS) for r in range(0, PW, ROWS)):
            m0, m1, m2 = (jnp.broadcast_to(mt[rows, k : k + 1], (ROWS, 128)) for k in range(3))
            turns = m0 * place[0:1, :] + m1 * place[1:2, :] + m2 * place[2:3, :]
            cos, sin = circle(turns)
            phases = (cos, m0 * sin, m1 * sin, m2 * sin)
            for k in range(3):
                amp = rad3[rows, 128 * k : 128 * (k + 1)]
                for t in range(4):
                    ch = 4 * k + t
                    beta[slot, rows, 128 * ch : 128 * (ch + 1)] = (amp * phases[t]).astype(BF16)

    def project(yy, slot):
        acc[...] += dot(cbuf[yy], beta[slot])

    make_block(y, 7)

    blocks = [(y, 7)] + [((y + d) % NY, 6 - k) for k, d in enumerate(NEAR_FIRST)]

    def gathered(k):
        yy, slot = blocks[k]
        if k:
            remote(cbuf.at[yy], cbuf.at[yy], a_s, a_r.at[yy], (z, y, c, x)).wait_recv()
        project(yy, slot)

    for k in range(1, NY):
        yy, slot = blocks[k]
        remote(mbuf.at[yy], mbuf.at[yy], m_s, m_r.at[yy], (z, y, c, x)).wait_recv()
        if k >= LAG:
            gathered(k - LAG)
        make_block(yy, slot)
    for k in range(NY - LAG, NY):
        gathered(k)

    g32 = iota((32, 128), 1) >> 5

    def lane_tile(j, g):
        tile = jnp.zeros((32, 128), F32)
        for k in range(4):
            chan = acc[:, 128 * (4 * g + k) : 128 * (4 * g + k + 1)]
            if k != j:
                chan = pltpu.roll(chan, (32 * (k - j)) % 128, 1)
            tile = jnp.where(g32 == k, chan, tile)
        return tile

    stacked = jnp.concatenate(
        [jnp.concatenate([lane_tile(j, g) for g in range(3)], axis=1) for j in range(4)], axis=0
    ).T.astype(BF16)
    rs_send[...] = dot(perm[...], stacked).astype(BF16).reshape(16, 24, 128)
    sid = c * NZ + z
    for d in FAR_FIRST:
        for o in range(NC):
            zz, cc = (z + d) % NZ, (c + o) % NC
            remote(rs_send.at[cc * NZ + zz], rs_recv.at[sid], rs_s, rs_r, (zz, y, cc, x)).start()
    remote(rs_send.at[(1 - c) * NZ + z], rs_recv.at[sid], rs_s, rs_r, (z, y, 1 - c, x)).start()

    near = 2 * c + 1 - x % 2
    which = jnp.where((near + 1) % NX == x, 0, 1)
    for cs in range(2):
        spot, sem = half_of(near, cs, which)
        remote(spot, spot, b_s.at[0], b_r.at[sem], (z, y, c, x)).wait_recv()
        remote(spot, spot, b_s.at[2], b_r.at[sem], (z, y, c, (near + 2) % NX)).start()

    def received(buf, sem):
        remote(buf, buf, rs_s, sem, (z, y, c, x)).wait_recv()

    def sent(buf, sem):
        remote(buf, buf, sem, rs_r, (z, y, c, x)).wait_send()

    received(rs_recv.at[0:15], rs_r)
    total = rs_send[sid].astype(F32)
    for d in range(NZ):
        for o in range(NC):
            if d or o:
                total = total + rs_recv[((c + o) % NC) * NZ + (z + d) % NZ].astype(F32)

    fm = z + c * (y - z)
    sm = y + c * (z - y)

    def at_first(f):
        return (z + (1 - c) * (f - z), y + c * (f - y), c, x)

    def at_second(s):
        return (z + c * (s - z), y + (1 - c) * (s - y), c, x)

    nbuf[sm, 0] = total.astype(BF16)
    for d in FAR_FIRST:
        k = PLACE[(8 - d) % 8]
        remote(nbuf.at[sm, 0], nbuf.at[sm, k], g1_s, g1_r.at[BATCH_OF[k]], at_first((fm + d) % 8)).start()
    for batch, (low, high) in enumerate(BATCHES):
        if batch:
            received(nbuf.at[sm, low:high], g1_r.at[batch])
        rows = nbuf.at[sm, low:high]
        for d in FAR_FIRST:
            remote(rows, rows, g2_s, g2_r.at[sm], at_second((sm + d) % 8)).start()

    group = iota((24, 128), 1) >> 5

    masks = [(group == j).astype(F32).astype(BF16) for j in range(4)]

    def spread_row(s):
        for k in range(8):
            f = (fm + ((k + 1) // 2 if k % 2 else 8 - k // 2)) % 8
            zz = f + c * (s - f)
            yy = s + c * (f - s)
            n = (zz // 2) * 16 + yy * 2 + zz % 2
            piece = nbuf[s, k]
            for j in range(4):
                wide[n, 24 * j : 24 * (j + 1), :] = piece * masks[j]

    spread_row(sm)
    for d in NEAR_FIRST:
        ss = (sm + d) % 8
        received(nbuf.at[ss], g2_r.at[ss])
        spread_row(ss)

    for xh in range(2):
        for cs in range(2):
            for h in range(2):
                xs = 2 * c + xh
                mine = (xs == x) & (c == cs)
                passed = (xs == near) & (which == h)
                spot, sem = half_of(xs, cs, h)

                @pl.when(mine)
                def _():
                    own_copies[h].wait()

                @pl.when(jnp.logical_not(mine | passed))
                def _():
                    remote(spot, spot, b_s.at[0], b_r.at[sem], (z, y, c, x)).wait_recv()

    def product(r):
        rows = pl.ds(pl.multiple_of(96 * r, 32), 96)
        part = jnp.zeros((96, 128), F32)
        for xh in range(2):
            part = part + dot(ball[xh, rows], wide[32 * xh : 32 * (xh + 1)].reshape(3072, 128))
        part = fold(part)
        pack = part[0:24]
        for k in range(1, 4):
            pack = jnp.where(group == k, part[24 * k : 24 * (k + 1)], pack)
        return pack

    xsend[...] = product(1 - c)
    xcp = remote(xsend, xrecv, x_s, x_r, (z, y, 1 - c, x))
    xcp.start()
    own = product(c)
    xcp.wait()
    qm = 2 * z + c
    mx[qm] = (own + xrecv[...]).astype(BF16)

    for d in FAR_FIRST:
        for o in range(NC):
            zz, cc = (z + d) % NZ, (c + o) % NC
            remote(mx.at[qm], mx.at[qm], e_s, e_r, (zz, y, cc, x)).start()
    remote(mx.at[qm], mx.at[qm], e_s, e_r, (z, y, 1 - c, x)).start()
    received(mx.at[0:15], e_r)

    ours = dot(back[...], mx[...].reshape(384, 128))
    ours = ours.T

    def channel(k):
        tile = jnp.zeros((32, 128), F32)
        for j in range(4):
            part = ours[32 * j : 32 * (j + 1), 128 * (k // 4) : 128 * (k // 4 + 1)]
            if k % 4 != j:
                part = pltpu.roll(part, (32 * (j - k % 4)) % 128, 1)
            tile = jnp.where(g32 == j, part, tile)
        return tile

    lhs = jnp.concatenate([channel(k) for k in range(NCH)], axis=1).astype(BF16)

    for low, high in GROUPS:
        both = lax.dot_general(
            lhs, beta[low:high].reshape((high - low) * PW, WIDTH),
            (((1,), (1,)), ((), ())), preferred_element_type=F32,
        )
        for slot in range(low, high):
            total = both[:, PW * (slot - low) : PW * (slot - low + 1)]
            if slot == 7:
                break
            d = FAR_FIRST[slot]
            yy = (y + d) % NY
            fsend[slot] = total.astype(BF16)
            remote(fsend.at[slot], frecv.at[y], f_s, f_r, (z, yy, c, x)).start()
    received(frecv.at[0:7], f_r)
    for d in NEAR_FIRST:
        total = total + frecv[(y + d) % NY].astype(F32)
    out[...] = total

    sent(cbuf.at[0:7], a_s)
    sent(mbuf.at[0:7], m_s)
    sent(ball.at[0], b_s.at[0])
    sent(ball.at[0, 0:96], b_s.at[2])
    sent(rs_send.at[0:15], rs_s)
    sent(nbuf.at[0, 0:7], g1_s)
    sent(nbuf.at[0:7], g2_s)
    sent(mx.at[0:15], e_s)
    sent(fsend.at[0:7], f_s)

    @pl.when(side != c)
    def _():
        sent(ball.at[0, 0:96], b_s.at[1])


def shards(coeffs, coupling, miller, species, proj_atom, positions, radial):
    vmem = pl.BlockSpec(memory_space=pltpu.VMEM)
    dma = pltpu.SemaphoreType.DMA
    inputs = (
        coeffs.T, miller, proj_atom.reshape(96, 128), species.reshape(1, ATOMS), positions, radial, coupling
    )
    change = pl.pallas_call(
        kernel,
        out_shape=jax.ShapeDtypeStruct((BANDS, PW), F32),
        in_specs=[pl.BlockSpec(memory_space=pl.ANY)] * 7,
        out_specs=vmem,
        scratch_shapes=[
            pltpu.VMEM((3, PW), jnp.int32),
            pltpu.VMEM((96, 128), jnp.int32),
            pltpu.VMEM((1, ATOMS), jnp.int32),
            pltpu.VMEM((3, ATOMS), F32),
            pltpu.VMEM((12, QBINS), F32),
            dma((6,)),
            pltpu.VMEM((NY, BANDS, PW), BF16),
            pltpu.VMEM((NY, 8, PW), BF16),
            pltpu.VMEM((8, PW), F32),
            pltpu.VMEM((NY, PW, WIDTH), BF16),
            pltpu.VMEM((BANDS, WIDTH), F32),
            pltpu.VMEM((3, 128), F32),
            pltpu.VMEM((PW, 384), F32),
            pltpu.VMEM((384, 384), BF16),
            pltpu.VMEM((384, 384), BF16),
            pltpu.VMEM((384, 384), BF16),
            pltpu.VMEM((16, 24, 128), BF16),
            pltpu.VMEM((16, 24, 128), BF16),
            pltpu.VMEM((8, 8, 24, 128), BF16),
            pltpu.VMEM((64, 96, 128), BF16),
            pltpu.VMEM((2, 192, 3072), BF16),
            pltpu.VMEM((24, 128), F32),
            pltpu.VMEM((24, 128), F32),
            pltpu.VMEM((16, 24, 128), BF16),
            pltpu.VMEM((NY, BANDS, PW), BF16),
            pltpu.VMEM((NY, BANDS, PW), BF16),
            dma, dma((8,)), dma, dma((8,)), dma, dma, dma, dma((4,)), dma, dma((8,)),
            dma((3,)), dma((8,)), dma((2,)), dma, dma, dma, dma, dma, dma,
        ],
        compiler_params=pltpu.CompilerParams(
            collective_id=0, has_side_effects=True, vmem_limit_bytes=48 * 1024 * 1024
        ),
    )(
        *(pltpu.with_memory_space_constraint(v, pltpu.HBM) for v in inputs)
    )
    return (coeffs.T.astype(F32) + change).astype(BF16).T


def solution(mesh):
    torus = Mesh(mesh.devices.reshape(NZ, NY, NC, NX), ("z", "y", "core", "band"))
    return jax.shard_map(
        shards,
        mesh=torus,
        in_specs=(P(GA, "band"), P(GA, "band"), P(None, GA), P(), P(), P(), P()),
        out_specs=P(GA, "band"),
        check_vma=False,
    )
```

```python
import math

import jax
import jax.numpy as jnp
from jax import lax
from jax.experimental import pallas as pl
from jax.experimental.pallas import tpu as pltpu
from jax.sharding import Mesh
from jax.sharding import PartitionSpec as P

NCH = 12
QBINS = 128
MMAX = 24
GA = ("z", "y", "core")
NZ, NY, NC, NX = 8, 8, 2, 4
PW = 256
BANDS = 32
ATOMS = 1024
LANE_ATOMS = 128
ROWS = 64
WIDTH = LANE_ATOMS * NCH
HALF = 6144
SCALE = 1.0 / math.sqrt(32768.0)
MESH = pl.DeviceIdType.MESH
FAR_FIRST = (4, 5, 3, 6, 2, 7, 1)
NEAR_FIRST = (1, 7, 2, 6, 3, 5, 4)
PLACE = {0: 0, 1: 1, 7: 2, 2: 3, 6: 4, 3: 5, 5: 6, 4: 7}
BATCHES = ((0, 1), (1, 3), (3, 5), (5, 8))
BATCH_OF = (0, 1, 1, 2, 2, 3, 3, 3)
F32 = jnp.float32
BF16 = jnp.bfloat16


def dot(a, b, **kw):
    return jnp.dot(a, b, preferred_element_type=F32, **kw)


def split2(v):
    hi = v.astype(BF16)
    return hi, (v - hi.astype(F32)).astype(BF16)


def iota(shape, dim):
    return lax.broadcasted_iota(jnp.int32, shape, dim)


def horner(y, terms):
    acc = jnp.full_like(y, terms[-1])
    for term in terms[-2::-1]:
        acc = acc * y + term
    return acc


SIN_TERMS = (
    3.141590270206989,
    -5.167406733272336,
    2.544010518503403,
    -0.5594624554679108,
)
COS_TERMS = (
    0.9999999532476079,
    -4.934792830619647,
    4.058411352862676,
    -1.3318765680812747,
    0.21968961109860236,
)


def circle(turns):
    r = turns - jnp.floor(turns + 0.5)
    y = r * r
    s = r * horner(y, SIN_TERMS)
    return 1.0 - 2.0 * (s * s), s * (horner(y, [t * (2.0 / MMAX) for t in COS_TERMS]))


def fold(v):
    v = v + pltpu.roll(v, 32, 1)
    return v + pltpu.roll(v, 64, 1)


def kernel(
    coeffs_h, miller_h, owner_h, species_h, positions_h, radial_h, coupling, out,
    miller, owner, species, positions, radial, in_s, cbuf, mtmp, beta, acc, place, rad3, rad_top, rad_low, perm, back,
    rs_send, rs_recv, nbuf, wide, ball, xsend, xrecv, mx, fsend, frecv,
    a_s, a_r, rs_s, rs_r, g1_s, g1_r, g2_s, g2_r, b_s, b_r, b_l, x_s, x_r, e_s, e_r, f_s, f_r,
):
    z, y, c, x = (lax.axis_index(a) for a in ("z", "y", "core", "band"))
    barrier = pltpu.get_barrier_semaphore()

    loads = [
        pltpu.make_async_copy(src, dst, in_s.at[k])
        for k, (src, dst) in enumerate(
            (
                (miller_h, miller), (coeffs_h, cbuf.at[y, 0:32]), (owner_h, owner),
                (radial_h, radial), (positions_h, positions), (species_h, species),
            )
        )
    ]
    for cp in loads[:2]:
        cp.start()

    def signal(to):
        pl.semaphore_signal(barrier, inc=1, device_id=to, device_id_type=MESH)

    for d in FAR_FIRST:
        signal((z, (y + d) % NY, c, x))
        for o in range(NC):
            signal(((z + d) % NZ, y, (c + o) % NC, x))
    for d in (2, 1, 3):
        for o in range(NC):
            signal((z, y, (c + o) % NC, (x + d) % NX))
    signal((z, y, 1 - c, x))
    greeted = 7 + 14 + 6 + 1

    def remote(src, dst, s, r, to):
        return pltpu.make_async_remote_copy(
            src_ref=src, dst_ref=dst, send_sem=s, recv_sem=r, device_id=to, device_id_type=MESH
        )
    for cp in loads[2:]:
        cp.start()
    def moved(natural, ours):
        atom_of = jnp.floor((natural.astype(F32) + 0.5) * (1.0 / NCH)).astype(jnp.int32)
        return (ours == (natural - NCH * atom_of) * 32 + atom_of).astype(F32).astype(BF16)

    square = (384, 384)
    perm[...] = moved(iota(square, 0), iota(square, 1))
    back[...] = moved(iota(square, 1), iota(square, 0))
    acc[...] = jnp.zeros_like(acc)

    for cp in loads[:2]:
        cp.wait()

    mtmp[...] = jnp.zeros_like(mtmp)
    mtmp[0:3, :] = miller[...].astype(F32)
    cbuf[y, 32:40, :] = mtmp[...].astype(BF16)

    for cp in loads[2:]:
        cp.wait()
    col = iota((128, 128), 1)
    j, q, i = col >> 5, (col >> 1) & 15, col & 1
    first = NCH * ((((q >> 1) * NY + y) * NC + (q & 1)) * 8 + j * 2 + i)
    row_of, lane_of = first >> 7, first & 127
    ids = owner[...].astype(F32).T
    ids_hi = jnp.floor(ids * (1.0 / 32.0))
    ids_lo = ids - 32.0 * ids_hi
    pick = (iota((128, 128), 0) == row_of).astype(F32)[0:96, :].astype(BF16)
    at_row = 32.0 * dot(ids_hi.astype(BF16), pick) + dot(ids_lo.astype(BF16), pick)
    atom = jnp.sum(jnp.where(iota((128, 128), 0) == lane_of, at_row, 0.0), axis=0, keepdims=True)
    onehot = (iota((ATOMS, 128), 0) == atom.astype(jnp.int32)).astype(F32)
    place[...] = dot(positions[...], onehot, precision=lax.Precision.HIGHEST)
    kind = dot(species[...].astype(F32).astype(BF16), onehot.astype(BF16))

    rsel = ((iota((128, 12), 0) & 15) == iota((128, 12), 1)).astype(F32)
    rad = dot(rsel, radial[...], precision=lax.Precision.HIGHEST).T * SCALE
    kind3 = 3 * kind.astype(jnp.int32)
    row = iota((128, 128), 0)
    pick_s = jnp.concatenate([(row == kind3 + k).astype(F32) for k in range(3)], axis=1)
    hi, lo = split2(dot(rad, pick_s, precision=lax.Precision.HIGHEST))
    rad_top[0:128, :] = hi
    rad_top[128:256, :] = hi
    rad_low[...] = lo

    pl.semaphore_wait(barrier, greeted)

    for d in NEAR_FIRST:
        yy = (y + d) % NY
        remote(cbuf.at[y], cbuf.at[y], a_s, a_r.at[y], (z, yy, c, x)).start()

    side = x // 2

    def half_of(xs, cs, h):
        return ball.at[xs % 2, pl.ds(96 * cs + 48 * h, 48)], 4 * (xs % 2) + 2 * cs + h

    own_copies, partner_copies = [], []
    for first in range(2):
        for way, dx in enumerate((1, 3)):
            h = first if way == 0 else 1 - first
            spot, sem = half_of(x, c, h)
            cp = remote(
                coupling.at[48 * h : 48 * (h + 1)], spot, b_s.at[0], b_r.at[sem], (z, y, side, (x + dx) % NX)
            )
            cp.start()
    for h in range(2):
        spot, sem = half_of(x, c, h)
        rows = coupling.at[48 * h : 48 * (h + 1)]
        own_copies.append(pltpu.make_async_copy(rows, spot, b_l.at[h]))
        partner_copies.append(remote(rows, spot, b_s.at[1], b_r.at[sem], (z, y, 1 - c, x)))

    @pl.when(side == c)
    def _():
        for cp in own_copies:
            cp.start()

    @pl.when(side != c)
    def _():
        for cp in partner_copies:
            cp.start()

    def make_block(yy, slot):
        m8 = cbuf[yy, 32:40, :].astype(F32)
        n2 = jnp.sum(m8 * m8, axis=0, keepdims=True)
        qv = n2 * ((QBINS - 1) / (3.0 * MMAX * MMAX))
        mt = jnp.where(iota((8, PW), 0) == 3, qv, m8).T
        hats = jnp.maximum(0.0, 1.0 - jnp.abs(mt[:, 3:4] - iota((PW, 128), 1).astype(F32)))
        h_hi, h_lo = split2(hats)
        rad3[...] = dot(jnp.concatenate([h_hi, h_lo], axis=1), rad_top[...]) + dot(h_hi, rad_low[...])
        for rows in (slice(r, r + ROWS) for r in range(0, PW, ROWS)):
            m0, m1, m2 = (jnp.broadcast_to(mt[rows, k : k + 1], (ROWS, 128)) for k in range(3))
            turns = m0 * place[0:1, :] + m1 * place[1:2, :] + m2 * place[2:3, :]
            cos, sin = circle(turns)
            phases = (cos, m0 * sin, m1 * sin, m2 * sin)
            for k in range(3):
                amp = rad3[rows, 128 * k : 128 * (k + 1)]
                for t in range(4):
                    ch = 4 * k + t
                    beta[slot, rows, 128 * ch : 128 * (ch + 1)] = (amp * phases[t]).astype(BF16)

    def project(yy, slot):
        acc[...] += dot(cbuf[yy, 0:32, :], beta[slot])

    make_block(y, 7)

    last = (y, 7)
    for k, d in enumerate(NEAR_FIRST):
        yy = (y + d) % NY
        remote(cbuf.at[yy], cbuf.at[yy], a_s, a_r.at[yy], (z, y, c, x)).wait_recv()
        project(*last)
        last = (yy, 6 - k)
        make_block(*last)
    project(*last)

    g32 = iota((32, 128), 1) >> 5

    def lane_tile(j, g):
        tile = jnp.zeros((32, 128), F32)
        for k in range(4):
            chan = acc[:, 128 * (4 * g + k) : 128 * (4 * g + k + 1)]
            if k != j:
                chan = pltpu.roll(chan, (32 * (k - j)) % 128, 1)
            tile = jnp.where(g32 == k, chan, tile)
        return tile

    stacked = jnp.concatenate(
        [jnp.concatenate([lane_tile(j, g) for g in range(3)], axis=1) for j in range(4)], axis=0
    ).T.astype(BF16)
    rs_send[...] = dot(perm[...], stacked).astype(BF16).reshape(16, 24, 128)
    sid = c * NZ + z
    for d in FAR_FIRST:
        for o in range(NC):
            zz, cc = (z + d) % NZ, (c + o) % NC
            remote(rs_send.at[cc * NZ + zz], rs_recv.at[sid], rs_s, rs_r, (zz, y, cc, x)).start()
    remote(rs_send.at[(1 - c) * NZ + z], rs_recv.at[sid], rs_s, rs_r, (z, y, 1 - c, x)).start()

    near = 2 * c + 1 - x % 2
    which = jnp.where((near + 1) % NX == x, 0, 1)
    for cs in range(2):
        spot, sem = half_of(near, cs, which)
        remote(spot, spot, b_s.at[0], b_r.at[sem], (z, y, c, x)).wait_recv()
        remote(spot, spot, b_s.at[2], b_r.at[sem], (z, y, c, (near + 2) % NX)).start()

    def received(buf, sem):
        remote(buf, buf, rs_s, sem, (z, y, c, x)).wait_recv()

    def sent(buf, sem):
        remote(buf, buf, sem, rs_r, (z, y, c, x)).wait_send()

    received(rs_recv.at[0:15], rs_r)
    total = rs_send[sid].astype(F32)
    for d in range(NZ):
        for o in range(NC):
            if d or o:
                total = total + rs_recv[((c + o) % NC) * NZ + (z + d) % NZ].astype(F32)

    fm = z + c * (y - z)
    sm = y + c * (z - y)

    def at_first(f):
        return (z + (1 - c) * (f - z), y + c * (f - y), c, x)

    def at_second(s):
        return (z + c * (s - z), y + (1 - c) * (s - y), c, x)

    nbuf[sm, 0] = total.astype(BF16)
    for d in FAR_FIRST:
        k = PLACE[(8 - d) % 8]
        remote(nbuf.at[sm, 0], nbuf.at[sm, k], g1_s, g1_r.at[BATCH_OF[k]], at_first((fm + d) % 8)).start()
    for batch, (low, high) in enumerate(BATCHES):
        if batch:
            received(nbuf.at[sm, low:high], g1_r.at[batch])
        rows = nbuf.at[sm, low:high]
        for d in FAR_FIRST:
            remote(rows, rows, g2_s, g2_r.at[sm], at_second((sm + d) % 8)).start()

    group = iota((24, 128), 1) >> 5

    masks = [(group == j).astype(F32).astype(BF16) for j in range(4)]

    def spread_row(s):
        for k in range(8):
            f = (fm + ((k + 1) // 2 if k % 2 else 8 - k // 2)) % 8
            zz = f + c * (s - f)
            yy = s + c * (f - s)
            n = (zz // 2) * 16 + yy * 2 + zz % 2
            piece = nbuf[s, k]
            for j in range(4):
                wide[n, 24 * j : 24 * (j + 1), :] = piece * masks[j]

    spread_row(sm)
    for d in NEAR_FIRST:
        ss = (sm + d) % 8
        received(nbuf.at[ss], g2_r.at[ss])
        spread_row(ss)

    for xh in range(2):
        for cs in range(2):
            for h in range(2):
                xs = 2 * c + xh
                mine = (xs == x) & (c == cs)
                passed = (xs == near) & (which == h)
                spot, sem = half_of(xs, cs, h)

                @pl.when(mine)
                def _():
                    own_copies[h].wait()

                @pl.when(jnp.logical_not(mine | passed))
                def _():
                    remote(spot, spot, b_s.at[0], b_r.at[sem], (z, y, c, x)).wait_recv()

    def product(r):
        rows = pl.ds(pl.multiple_of(96 * r, 32), 96)
        part = jnp.zeros((96, 128), F32)
        for xh in range(2):
            part = part + dot(ball[xh, rows], wide[32 * xh : 32 * (xh + 1)].reshape(3072, 128))
        part = fold(part)
        pack = part[0:24]
        for k in range(1, 4):
            pack = jnp.where(group == k, part[24 * k : 24 * (k + 1)], pack)
        return pack

    xsend[...] = product(1 - c)
    xcp = remote(xsend, xrecv, x_s, x_r, (z, y, 1 - c, x))
    xcp.start()
    own = product(c)
    xcp.wait()
    qm = 2 * z + c
    mx[qm] = (own + xrecv[...]).astype(BF16)

    for d in FAR_FIRST:
        for o in range(NC):
            zz, cc = (z + d) % NZ, (c + o) % NC
            remote(mx.at[qm], mx.at[qm], e_s, e_r, (zz, y, cc, x)).start()
    remote(mx.at[qm], mx.at[qm], e_s, e_r, (z, y, 1 - c, x)).start()
    received(mx.at[0:15], e_r)

    ours = dot(back[...], mx[...].reshape(384, 128))
    ours = ours.T

    def channel(k):
        tile = jnp.zeros((32, 128), F32)
        for j in range(4):
            part = ours[32 * j : 32 * (j + 1), 128 * (k // 4) : 128 * (k // 4 + 1)]
            if k % 4 != j:
                part = pltpu.roll(part, (32 * (j - k % 4)) % 128, 1)
            tile = jnp.where(g32 == j, part, tile)
        return tile

    lhs = jnp.concatenate([channel(k) for k in range(NCH)], axis=1).astype(BF16)

    for pair in range(4):
        both = lax.dot_general(
            lhs, beta[2 * pair : 2 * pair + 2].reshape(2 * PW, WIDTH),
            (((1,), (1,)), ((), ())), preferred_element_type=F32,
        )
        for half in range(2):
            total = both[:, PW * half : PW * (half + 1)]
            slot = 2 * pair + half
            if slot == 7:
                break
            d = FAR_FIRST[slot]
            yy = (y + d) % NY
            fsend[slot] = total.astype(BF16)
            remote(fsend.at[slot], frecv.at[y], f_s, f_r, (z, yy, c, x)).start()
    received(frecv.at[0:7], f_r)
    for d in NEAR_FIRST:
        total = total + frecv[(y + d) % NY].astype(F32)
    out[...] = total

    sent(cbuf.at[0:7], a_s)
    sent(ball.at[0], b_s.at[0])
    sent(ball.at[0, 0:96], b_s.at[2])
    sent(rs_send.at[0:15], rs_s)
    sent(nbuf.at[0, 0:7], g1_s)
    sent(nbuf.at[0:7], g2_s)
    sent(mx.at[0:15], e_s)
    sent(fsend.at[0:7], f_s)

    @pl.when(side != c)
    def _():
        sent(ball.at[0, 0:96], b_s.at[1])


def shards(coeffs, coupling, miller, species, proj_atom, positions, radial):
    vmem = pl.BlockSpec(memory_space=pltpu.VMEM)
    dma = pltpu.SemaphoreType.DMA
    inputs = (
        coeffs.T, miller, proj_atom.reshape(96, 128), species.reshape(1, ATOMS), positions, radial, coupling
    )
    change = pl.pallas_call(
        kernel,
        out_shape=jax.ShapeDtypeStruct((BANDS, PW), F32),
        in_specs=[pl.BlockSpec(memory_space=pl.ANY)] * 7,
        out_specs=vmem,
        scratch_shapes=[
            pltpu.VMEM((3, PW), jnp.int32),
            pltpu.VMEM((96, 128), jnp.int32),
            pltpu.VMEM((1, ATOMS), jnp.int32),
            pltpu.VMEM((3, ATOMS), F32),
            pltpu.VMEM((12, QBINS), F32),
            dma((6,)),
            pltpu.VMEM((NY, 40, PW), BF16),
            pltpu.VMEM((8, PW), F32),
            pltpu.VMEM((NY, PW, WIDTH), BF16),
            pltpu.VMEM((BANDS, WIDTH), F32),
            pltpu.VMEM((3, 128), F32),
            pltpu.VMEM((PW, 384), F32),
            pltpu.VMEM((256, 384), BF16),
            pltpu.VMEM((128, 384), BF16),
            pltpu.VMEM((384, 384), BF16),
            pltpu.VMEM((384, 384), BF16),
            pltpu.VMEM((16, 24, 128), BF16),
            pltpu.VMEM((16, 24, 128), BF16),
            pltpu.VMEM((8, 8, 24, 128), BF16),
            pltpu.VMEM((64, 96, 128), BF16),
            pltpu.VMEM((2, 192, 3072), BF16),
            pltpu.VMEM((24, 128), F32),
            pltpu.VMEM((24, 128), F32),
            pltpu.VMEM((16, 24, 128), BF16),
            pltpu.VMEM((NY, BANDS, PW), BF16),
            pltpu.VMEM((NY, BANDS, PW), BF16),
            dma, dma((8,)), dma, dma, dma, dma((4,)), dma, dma((8,)),
            dma((3,)), dma((8,)), dma((2,)), dma, dma, dma, dma, dma, dma,
        ],
        compiler_params=pltpu.CompilerParams(
            collective_id=0, has_side_effects=True, vmem_limit_bytes=48 * 1024 * 1024
        ),
    )(
        *(pltpu.with_memory_space_constraint(v, pltpu.HBM) for v in inputs)
    )
    return (coeffs.T.astype(F32) + change).astype(BF16).T


def solution(mesh):
    torus = Mesh(mesh.devices.reshape(NZ, NY, NC, NX), ("z", "y", "core", "band"))
    return jax.shard_map(
        shards,
        mesh=torus,
        in_specs=(P(GA, "band"), P(GA, "band"), P(None, GA), P(), P(), P(), P()),
        out_specs=P(GA, "band"),
        check_vma=False,
    )
```
